256 devices in a mesh: blk: 64 (over x, z, core), grp: 4 (over y).
Axes of the slice: x: 4, y: 4, z: 8, core: 2. Of those that a mesh axis runs over, the one named last changes fastest.
Arguments:
- source_coords: float32 [3, 163840], P(None, ('blk', 'grp')), may hold values from 0 to 64, as said below
- source_values: float32 [3, 163840], P(None, ('blk', 'grp')), may hold values from -48 to 48
- target_coords: float32 [3, 131072], P(None, ('blk', 'grp')), may hold values from 0 to 64, as said below
- target_owner: int32 [131072], P(('blk', 'grp')), may hold values from 0 to 63, as said below
Outputs:
- weights: float32 [3, 163840], P(None, ('blk', 'grp'))
- poly: float32 [3, 4], replicated
- mapped: float32 [3, 131072], P(None, ('blk', 'grp'))
The draws below stay inside these ranges and needn't reach their ends.
Inputs may be any that keep to these rules, and one draw needn't show every extreme that they name: `source_coords`: source vertex j has its first coordinate between j // 2560 and j // 2560 + 1, and the other two between 0 and 1. `target_coords`: target vertex t has its first coordinate between target_owner[t] and target_owner[t] + 1, and the other two between 0 and 1. target_owner[t] differs from t // 2048 by at most one.
All inputs are finite; a program needn't handle non-finite values.
Results may differ from the reference program's by a relative error of at most 0.0003.
Values sent between devices are 32-bit elements; how exact they have to be, the bound alone decides.
A program may use at most 64 MiB of HBM per device.

```python
import math
import jax
import jax.numpy as jnp
from jax import lax

C = 3
ITERS = 3
REACH = 2
TGT_DEV = 512
SLAB = 2560
NSRC = 163840
NTGT = 131072
N_BLK = 64
N_GRP = 4


def spread_draw(key, count):
    spread = jax.random.uniform(key, (3, count), jnp.float32)
    return spread


def source_layout(key):
    count = SLAB * N_BLK
    slab = (jnp.arange(count, dtype=jnp.int32) // SLAB).astype(jnp.float32)
    spread = spread_draw(jax.random.fold_in(key, 101), count)
    return jnp.stack([slab + spread[0], spread[1], spread[2]])


def draw_source_coords(key, part):
    return source_layout(key)


def draw_source_values(key, part):
    coords = source_layout(key)
    count = coords.shape[1]
    ones = jnp.ones_like(coords[0])
    basis_rows = jnp.stack([ones, 2.0 * coords[0] / N_BLK - 1.0, 2.0 * coords[1] - 1.0, 2.0 * coords[2] - 1.0])
    rising = 1.0 + 2.0 * coords[0] / N_BLK
    trend = jax.random.uniform(jax.random.fold_in(key, 202), (C, 4), jnp.float32, -1.5, 1.5)
    rough = jnp.clip(jax.random.normal(jax.random.fold_in(key, 203), (C, count), jnp.float32), -4.0, 4.0)
    return jnp.dot(trend, basis_rows) + rising[None, :] * rough


def target_layout(key):
    count = TGT_DEV * N_GRP * N_BLK
    home = jnp.arange(count, dtype=jnp.int32) // (TGT_DEV * N_GRP)
    offset = jax.random.randint(jax.random.fold_in(key, 303), (count,), -1, 2)
    return jnp.clip(home + offset, 0, N_BLK - 1)


def draw_target_owner(key, part):
    return target_layout(key).astype(jnp.int32)


def draw_target_coords(key, part):
    owner = target_layout(key).astype(jnp.float32)
    count = owner.shape[0]
    spread = spread_draw(jax.random.fold_in(key, 404), count)
    return jnp.stack([owner + spread[0], spread[1], spread[2]])


def setup_inputs(seed: int = 0) -> dict:
    key_of = jax.random.split(jax.random.key(seed), 5)
    source_coords = draw_source_coords(jax.random.fold_in(key_of[4], 71), 0)
    source_values = draw_source_values(jax.random.fold_in(key_of[4], 71), 0)
    target_coords = draw_target_coords(jax.random.fold_in(key_of[4], 71), 0)
    target_owner = draw_target_owner(jax.random.fold_in(key_of[4], 71), 0)
    return {"source_coords": source_coords, "source_values": source_values, "target_coords": target_coords, "target_owner": target_owner}


precise = lax.Precision.HIGHEST
thin_factor = 0.6
tiny = 1e-06

def kernel_tile(rows, cols, stretch):
    along = rows[0][None, :] - cols[0][:, None]
    across = rows[1][None, :] - cols[1][:, None]
    upward = rows[2][None, :] - cols[2][:, None]
    return jnp.exp(-(thin_factor * along * along + stretch * (across * across + upward * upward)))

def basis(points, partitions, sources):
    ones = jnp.ones_like(points[0])
    stacked = jnp.stack([ones, 2.0 * points[0] / partitions - 1.0, 2.0 * points[1] - 1.0, 2.0 * points[2] - 1.0])
    return stacked / math.sqrt(sources)

def least_squares(hessenberg, beta):
    count = len(hessenberg)
    right_side = [beta] + [jnp.zeros_like(beta) for k in range(count)]
    upper = []
    cosines = []
    sines = []
    for k in range(count):
        column = list(hessenberg[k])
        for i in range(k):
            top = cosines[i] * column[i] + sines[i] * column[i + 1]
            lower = -sines[i] * column[i] + cosines[i] * column[i + 1]
            column[i] = top
            column[i + 1] = lower
        radius = jnp.sqrt(column[k] * column[k] + column[k + 1] * column[k + 1])
        cosine = column[k] / radius
        sine = column[k + 1] / radius
        column[k] = radius
        cosines.append(cosine)
        sines.append(sine)
        right_side[k + 1] = -sine * right_side[k]
        right_side[k] = cosine * right_side[k]
        upper.append(column[:k + 1])
    solved = [None] * count
    for k in reversed(range(count)):
        running = right_side[k]
        for j in range(k + 1, count):
            running = running - upper[j][k] * solved[j]
        solved[k] = running / upper[k][k]
    return solved

def reference(source_coords, source_values, target_coords, target_owner):
    stretch = 4.0 * SLAB
    reach = REACH
    poly_src = basis(source_coords, N_BLK, NSRC)
    margin = reach * SLAB
    coords_pad = jnp.pad(source_coords, ((0, 0), (margin, margin)))

    def kernel_apply(head):
        head_pad = jnp.pad(head, ((0, 0), (margin, margin)))

        def one_slab(slab):
            start = (slab * SLAB).astype(jnp.int32)
            rows = lax.dynamic_slice_in_dim(source_coords, start, SLAB, 1)
            running = jnp.zeros((C, SLAB), jnp.float32)
            for offset in range(2 * reach + 1):
                begin = (start + offset * SLAB).astype(jnp.int32)
                cols = lax.dynamic_slice_in_dim(coords_pad, begin, SLAB, 1)
                values = lax.dynamic_slice_in_dim(head_pad, begin, SLAB, 1)
                running = running + jnp.dot(values, kernel_tile(rows, cols, stretch), precision=precise, preferred_element_type=jnp.float32)
            return running
        blocks = lax.map(one_slab, jnp.arange(N_BLK, dtype=jnp.int32))
        return jnp.transpose(blocks, (1, 0, 2)).reshape(C, NSRC)

    def operate(head, tail):
        image_head = kernel_apply(head) + jnp.dot(tail, poly_src, precision=precise, preferred_element_type=jnp.float32)
        image_tail = jnp.dot(head, poly_src.T, precision=precise, preferred_element_type=jnp.float32)
        return (image_head, image_tail)
    beta = jnp.sqrt(lax.optimization_barrier(jnp.sum(source_values * source_values, axis=1)) + tiny)
    heads = [source_values / beta[:, None]]
    tails = [jnp.zeros((C, 4), jnp.float32)]
    hessenberg = []
    for k in range(ITERS):
        image_head, image_tail = operate(heads[k], tails[k])
        column = []
        for i in range(k + 1):
            column.append(lax.optimization_barrier(jnp.sum(heads[i] * image_head, axis=1)) + lax.optimization_barrier(jnp.sum(tails[i] * image_tail, axis=1)))
        rest_head = image_head
        rest_tail = image_tail
        for i in range(k + 1):
            rest_head = rest_head - column[i][:, None] * heads[i]
            rest_tail = rest_tail - column[i][:, None] * tails[i]
        length = jnp.sqrt(lax.optimization_barrier(jnp.sum(rest_head * rest_head, axis=1)) + lax.optimization_barrier(jnp.sum(rest_tail * rest_tail, axis=1)) + tiny)
        column.append(length)
        hessenberg.append(column)
        heads.append(rest_head / length[:, None])
        tails.append(rest_tail / length[:, None])
    solved = least_squares(hessenberg, beta)
    weights = solved[0][:, None] * heads[0]
    poly = solved[0][:, None] * tails[0]
    for k in range(1, ITERS):
        weights = weights + solved[k][:, None] * heads[k]
        poly = poly + solved[k][:, None] * tails[k]
    poly_tgt = basis(target_coords, N_BLK, NSRC)
    wide = (reach + 1) * SLAB
    coords_far = jnp.pad(source_coords, ((0, 0), (wide, wide)))
    weights_far = jnp.pad(weights, ((0, 0), (wide, wide)))
    group_rows = TGT_DEV * N_GRP

    def one_group(group):
        first = (group * group_rows).astype(jnp.int32)
        rows = lax.dynamic_slice_in_dim(target_coords, first, group_rows, 1)
        owners = lax.dynamic_slice_in_dim(target_owner, first, group_rows, 0)
        running = jnp.zeros((C, group_rows), jnp.float32)
        for offset in range(2 * reach + 3):
            slab = group + offset - reach - 1
            begin = ((group + offset) * SLAB).astype(jnp.int32)
            cols = lax.dynamic_slice_in_dim(coords_far, begin, SLAB, 1)
            values = lax.dynamic_slice_in_dim(weights_far, begin, SLAB, 1)
            tile = kernel_tile(rows, cols, stretch)
            tile = jnp.where((jnp.abs(owners - slab) <= reach)[None, :], tile, 0.0)
            running = running + jnp.dot(values, tile, precision=precise, preferred_element_type=jnp.float32)
        return running
    evaluated = lax.map(one_group, jnp.arange(N_BLK, dtype=jnp.int32))
    mapped = jnp.transpose(evaluated, (1, 0, 2)).reshape(C, NTGT)
    mapped = mapped + jnp.dot(poly, poly_tgt, precision=precise, preferred_element_type=jnp.float32)
    return (weights, poly, mapped)
```

```python
import functools
import math

import jax
import jax.numpy as jnp
from jax import lax
from jax.experimental import pallas as pl
from jax.experimental.pallas import tpu as pltpu
from jax.sharding import PartitionSpec as P

MESH = pl.DeviceIdType.MESH
ITERS = 3
REACH = 2
FAR = REACH + 1
NB = 64
NG = 4
RING = 16
OWN = 640
TGT = 512
LANE = 128
CH = OWN // LANE
SLAB = OWN * NG
NSRC = SLAB * NB
STRETCH = 4.0 * SLAB
SHIFT = 2.0
TINY = 1e-6
LOG2E = 1.4426950408889634
XSCALE = math.sqrt(0.6 * LOG2E)
YZ = -STRETCH * LOG2E
ROOT = 1.0 / math.sqrt(NSRC)
NEAR_SLOTS = (2 * REACH + 1) * NG
FAR_SLOTS = (2 * FAR + 1) * NG
SUB = 64
f32 = jnp.float32
bf16 = jnp.bfloat16
HIGH = lax.Precision.HIGHEST


def split(v):
    hi = v.astype(bf16)
    return hi, (v - hi.astype(f32)).astype(bf16)


def least_squares(hessenberg, beta):
    count = len(hessenberg)
    right_side = [beta] + [jnp.zeros_like(beta) for k in range(count)]
    upper = []
    cosines = []
    sines = []
    for k in range(count):
        column = list(hessenberg[k])
        for i in range(k):
            top = cosines[i] * column[i] + sines[i] * column[i + 1]
            lower = -sines[i] * column[i] + cosines[i] * column[i + 1]
            column[i] = top
            column[i + 1] = lower
        radius = jnp.sqrt(column[k] * column[k] + column[k + 1] * column[k + 1])
        cosine = column[k] / radius
        sine = column[k + 1] / radius
        column[k] = radius
        cosines.append(cosine)
        sines.append(sine)
        right_side[k + 1] = -sine * right_side[k]
        right_side[k] = cosine * right_side[k]
        upper.append(column[: k + 1])
    solved = [None] * count
    for k in reversed(range(count)):
        running = right_side[k]
        for j in range(k + 1, count):
            running = running - upper[j][k] * solved[j]
        solved[k] = running / upper[k][k]
    return solved


def basis_rows(x, y, z):
    return (
        jnp.full_like(x, ROOT),
        (2.0 * x / NB - 1.0) * ROOT,
        (2.0 * y - 1.0) * ROOT,
        (2.0 * z - 1.0) * ROOT,
    )


def coefficients(gram):
    lane = lax.broadcasted_iota(jnp.int32, (8, LANE), 1)
    row = lax.broadcasted_iota(jnp.int32, (8, LANE), 0)
    tail_lanes = (lane >= 12) & (lane < 16)

    def total(v):
        return jnp.sum(v, axis=1, keepdims=True)

    def times_gram(v):
        return jnp.dot(v, gram, precision=HIGH, preferred_element_type=f32)

    def shifted(v):
        up = pltpu.roll(v, 3, 1)
        across = pltpu.roll(v, 4, 1)
        moved = jnp.where(lane < 12, up, jnp.where((lane >= 16) & (lane < 20), across, 0.0))
        moved = jnp.where(lane < 3, 0.0, moved)
        return moved + SHIFT * v

    first = jnp.where((lane == row) & (row < 3), 1.0, 0.0)
    first_gram = times_gram(first)
    beta = jnp.sqrt(total(first_gram * first) + TINY)
    heads = [first / beta]
    tails = [jnp.zeros_like(first)]
    grams = [first_gram / beta]
    hessenberg = []
    for k in range(ITERS):
        head = shifted(heads[k]) + tails[k]
        tail = jnp.where(tail_lanes, grams[k], 0.0)
        head_gram = times_gram(head)
        column = [
            total(head_gram * heads[i]) + total(tail * tails[i]) for i in range(k + 1)
        ]
        for i in range(k + 1):
            head = head - column[i] * heads[i]
            tail = tail - column[i] * tails[i]
        rest_gram = times_gram(head)
        length = jnp.sqrt(total(rest_gram * head) + total(tail * tail) + TINY)
        column.append(length)
        hessenberg.append(column)
        heads.append(head / length)
        tails.append(tail / length)
        grams.append(rest_gram / length)
    solved = least_squares(hessenberg, beta)
    head = solved[0] * heads[0]
    tail = solved[0] * tails[0]
    for k in range(1, ITERS):
        head = head + solved[k] * heads[k]
        tail = tail + solved[k] * tails[k]
    return head, tail


def kernel(
    coords_ref,
    values_ref,
    tcoords_ref,
    owner_ref,
    weights_ref,
    poly_ref,
    mapped_ref,
    c0,
    f1,
    f2,
    kh,
    kl,
    th,
    tl,
    cb,
    rows,
    trows,
    fmat,
    mmat,
    ga,
    gb,
    send_sem,
    recv_sem,
    a_send,
    a_recv,
    b_send,
    b_recv,
):
    p = lax.axis_index("blk")
    g = lax.axis_index("grp")
    xi = p // RING
    zi = p % RING
    own = FAR * NG + g

    def valid(o):
        return (p + o >= 0) & (p + o < NB)

    halo = []
    for d in range(1, NG):
        halo.append((0, (g + d) % NG))
    for dist in range(1, FAR + 1):
        for o in (dist, -dist):
            for d in range(NG):
                halo.append((o, (g + d) % NG))
    ring_a = [(xi * RING + (zi + d) % RING, g) for d in range(1, RING)]
    ring_b = [
        (((xi + dx) % 4) * RING + zi, (g + dg) % NG)
        for dx in range(4)
        for dg in range(NG)
        if (dx, dg) != (0, 0)
    ]

    barrier = pltpu.get_barrier_semaphore()

    def signal(q, h):
        pl.semaphore_signal(barrier, inc=1, device_id=(q, h), device_id_type=MESH)

    expected = NG - 1 + len(ring_a) + len(ring_b)
    for o, h in halo:
        if o == 0:
            signal(p, h)
        else:
            pl.when(valid(o))(functools.partial(signal, p + o, h))
    for o in range(-FAR, FAR + 1):
        if o != 0:
            expected = expected + jnp.where(valid(o), NG, 0)
    for q, h in ring_a + ring_b:
        signal(q, h)

    for t in range(CH):
        lanes = slice(t * LANE, (t + 1) * LANE)
        c0[own, 3 * t : 3 * t + 3, :] = coords_ref[:, lanes]
        c0[own, 16 + 3 * t : 16 + 3 * t + 3, :] = values_ref[:, lanes]
    base = p.astype(f32)
    sx, sy, sz = coords_ref[0:1, :], coords_ref[1:2, :], coords_ref[2:3, :]
    rows[0:1, :] = (sx - base) * XSCALE
    rows[1:2, :] = sy
    rows[2:3, :] = sz
    fmat[...] = jnp.zeros_like(fmat)
    mmat[...] = jnp.zeros_like(mmat)
    fmat[0:3, :] = values_ref[...]
    for i, part in enumerate(basis_rows(sx, sy, sz)):
        fmat[12 + i : 13 + i, :] = part
    tx, ty, tz = tcoords_ref[0:1, :], tcoords_ref[1:2, :], tcoords_ref[2:3, :]
    owner = owner_ref[...]
    for o in range(-FAR, FAR + 1):
        inside = jnp.abs(owner - (p + o)) <= REACH
        trows[FAR + o] = jnp.where(inside, (tx - base) * XSCALE, 1e6)
    trows[7] = ty
    trows[8] = tz
    for i, part in enumerate(basis_rows(tx, ty, tz)):
        mmat[24 + i : 25 + i, :] = part

    absent = jnp.where(
        lax.broadcasted_iota(jnp.int32, (32, LANE), 0) % 3 == 0, 1e5, 0.0
    )
    absent = jnp.where(lax.broadcasted_iota(jnp.int32, (32, LANE), 0) < 15, absent, 0.0)
    for o in range(-FAR, FAR + 1):
        if o != 0:

            @pl.when(jnp.logical_not(valid(o)))
            def _():
                for h in range(NG):
                    slot = (FAR + o) * NG + h
                    c0[slot] = absent
                    f1[slot] = jnp.zeros((16, LANE), f32)
                    f2[slot] = jnp.zeros((16, LANE), f32)

    pl.semaphore_wait(barrier, expected)

    def block_copy(buf, which, o, h):
        return pltpu.make_async_remote_copy(
            src_ref=buf.at[own],
            dst_ref=buf.at[(FAR - o) * NG + g],
            send_sem=send_sem.at[which, (FAR + o) * NG + h],
            recv_sem=recv_sem.at[which, (FAR - o) * NG + g],
            device_id=(p + o, h),
            device_id_type=MESH,
        )

    def send_all(buf, which):
        for o, h in halo:
            copy = block_copy(buf, which, o, h)
            if o == 0:
                copy.start()
            else:
                pl.when(valid(o))(copy.start)

    def wait_send_all(buf, which):
        for o, h in halo:
            copy = block_copy(buf, which, o, h)
            if o == 0:
                copy.wait_send()
            else:
                pl.when(valid(o))(copy.wait_send)

    def wait_block(buf, which, o, h):
        slot = (FAR + o) * NG + h
        pltpu.make_async_remote_copy(
            src_ref=buf.at[own],
            dst_ref=buf.at[slot],
            send_sem=send_sem.at[which, slot],
            recv_sem=recv_sem.at[which, slot],
            device_id=(p + o, h),
            device_id_type=MESH,
        ).wait_recv()

    def place(k):
        oi = k // NG
        dist = (oi + 1) // 2
        o = jnp.where(oi % 2 == 1, dist, -dist)
        h = (g + k % NG) % NG
        return o, h, (FAR + o) * NG + h

    send_all(c0, 0)

    def column_coords(slot, t):
        cc = c0[slot, 3 * t : 3 * t + 3, :]
        sides = []
        for i in range(3):
            row = cc[i : i + 1, :]
            if i == 0:
                row = (row - base) * XSCALE
            sides.append(jnp.broadcast_to(row, (LANE, LANE)).T)
        for i in range(3):
            cb[t, i] = sides[i]

    def tile(t, sub, rx, ry, rz):
        at = slice(sub * SUB, (sub + 1) * SUB)
        dx = cb[t, 0, at, :] - rx
        dy = cb[t, 1, at, :] - ry
        dz = cb[t, 2, at, :] - rz
        return jnp.exp2(YZ * (dy * dy + dz * dz) - dx * dx)

    def near_values(slot, t):
        cc = c0[slot, 3 * t : 3 * t + 3, :]
        parts = [c0[slot, 16 + 3 * t : 16 + 3 * t + 3, :]]
        parts += basis_rows(cc[0:1], cc[1:2], cc[2:3])
        parts.append(jnp.zeros((1, LANE), f32))
        return jnp.concatenate(split(jnp.concatenate(parts, axis=0)), axis=0)

    def build(k, acc):
        o, h, slot = place(k)

        @pl.when((k > 0) & valid(o))
        def _():
            wait_block(c0, 0, o, h)

        start = pl.multiple_of(k * OWN, OWN)
        for t in range(CH):
            column_coords(slot, t)
        for t in range(CH):
            for n in range(OWN // LANE):
                lanes = slice(n * LANE, (n + 1) * LANE)
                rx, ry, rz = rows[0:1, lanes], rows[1:2, lanes], rows[2:3, lanes]
                for sub in range(LANE // SUB):
                    hi, lo = split(tile(t, sub, rx, ry, rz))
                    at = pl.ds(start + t * LANE + sub * SUB, SUB)
                    kh[at, lanes] = hi
                    kl[at, lanes] = lo
            v = near_values(slot, t)
            at = pl.ds(start + t * LANE, LANE)
            acc = acc + jnp.dot(v, kh[at, :], preferred_element_type=f32)
            acc = acc + jnp.dot(v, kl[at, :], preferred_element_type=f32)
        return acc

    acc = lax.fori_loop(0, NEAR_SLOTS, build, jnp.zeros((16, OWN), f32))
    image = acc[0:8] + acc[8:16]
    first = image[0:3] - SHIFT * fmat[0:3, :]
    fmat[3:6, :] = first
    fmat[16:20, :] = image[3:7] - SHIFT * fmat[12:16, :]

    def keep_own(buf, v):
        for t in range(CH):
            buf[own, 3 * t : 3 * t + 3, :] = v[:, t * LANE : (t + 1) * LANE]

    keep_own(f1, first)
    send_all(f1, 1)

    def padded_split(v):
        v = jnp.concatenate([v, jnp.zeros((5, LANE), f32)], axis=0)
        return jnp.concatenate(split(v), axis=0)

    def apply_near(buf, which):
        def step(k, acc):
            o, h, slot = place(k)

            @pl.when((k > 0) & valid(o))
            def _():
                wait_block(buf, which, o, h)

            start = pl.multiple_of(k * OWN, OWN)
            v = jnp.concatenate(
                [padded_split(buf[slot, 3 * t : 3 * t + 3, :]) for t in range(CH)], axis=1
            )
            at = pl.ds(start, OWN)
            acc = acc + jnp.dot(v, kh[at, :], preferred_element_type=f32)
            return acc + jnp.dot(v, kl[at, :], preferred_element_type=f32)

        acc = lax.fori_loop(0, NEAR_SLOTS, step, jnp.zeros((16, OWN), f32))
        return acc[0:3] + acc[8:11]

    second = apply_near(f1, 1) - SHIFT * first
    fmat[6:9, :] = second
    keep_own(f2, second)
    send_all(f2, 2)
    third = apply_near(f2, 2) - SHIFT * second
    fmat[9:12, :] = third

    everything = fmat[...]
    ga[zi] = lax.dot_general(
        fmat[0:24, :],
        everything,
        (((1,), (1,)), ((), ())),
        precision=HIGH,
        preferred_element_type=f32,
    )

    def a_copy(d):
        q, h = ring_a[d - 1]
        return pltpu.make_async_remote_copy(
            src_ref=ga.at[zi],
            dst_ref=ga.at[zi],
            send_sem=a_send.at[d],
            recv_sem=a_recv.at[zi],
            device_id=(q, h),
            device_id_type=MESH,
        )

    def a_wait(d):
        slot = (zi + d) % RING
        pltpu.make_async_remote_copy(
            src_ref=ga.at[zi],
            dst_ref=ga.at[slot],
            send_sem=a_send.at[d],
            recv_sem=a_recv.at[slot],
            device_id=ring_a[d - 1],
            device_id_type=MESH,
        ).wait_recv()

    me_b = xi * NG + g

    def b_copy(i):
        return pltpu.make_async_remote_copy(
            src_ref=gb.at[me_b],
            dst_ref=gb.at[me_b],
            send_sem=b_send.at[i],
            recv_sem=b_recv.at[me_b],
            device_id=ring_b[i],
            device_id_type=MESH,
        )

    def b_wait(i):
        dx, dg = (i + 1) // NG, (i + 1) % NG
        slot = ((xi + dx) % 4) * NG + (g + dg) % NG
        pltpu.make_async_remote_copy(
            src_ref=gb.at[me_b],
            dst_ref=gb.at[slot],
            send_sem=b_send.at[i],
            recv_sem=b_recv.at[slot],
            device_id=ring_b[i],
            device_id_type=MESH,
        ).wait_recv()

    for d in range(1, RING):
        a_copy(d).start()

    def far_values(slot, t):
        cc = c0[slot, 3 * t : 3 * t + 3, :]
        parts = [
            c0[slot, 16 + 3 * t : 16 + 3 * t + 3, :],
            f1[slot, 3 * t : 3 * t + 3, :],
            f2[slot, 3 * t : 3 * t + 3, :],
            jnp.zeros((3, LANE), f32),
        ]
        parts += basis_rows(cc[0:1], cc[1:2], cc[2:3])
        return jnp.concatenate(split(jnp.concatenate(parts, axis=0)), axis=0)

    def target(k, acc):
        o, h, slot = place(k)

        @pl.when((k >= NEAR_SLOTS) & valid(o))
        def _():
            wait_block(c0, 0, o, h)
            wait_block(f1, 1, o, h)
            wait_block(f2, 2, o, h)

        for t in range(CH):
            column_coords(slot, t)
        for t in range(CH):
            for n in range(TGT // LANE):
                lanes = slice(n * LANE, (n + 1) * LANE)
                rx = trows[FAR + o, :, lanes]
                ry, rz = trows[7, :, lanes], trows[8, :, lanes]
                for sub in range(LANE // SUB):
                    hi, lo = split(tile(t, sub, rx, ry, rz))
                    at = slice(t * LANE + sub * SUB, t * LANE + (sub + 1) * SUB)
                    th[at, lanes] = hi
                    tl[at, lanes] = lo
            v = far_values(slot, t)
            at = slice(t * LANE, (t + 1) * LANE)
            acc = acc + jnp.dot(v, th[at, :], preferred_element_type=f32)
            acc = acc + jnp.dot(v, tl[at, :], preferred_element_type=f32)
        return acc

    half = FAR_SLOTS // 2
    acc = lax.fori_loop(0, half, target, jnp.zeros((32, TGT), f32))

    for d in range(1, RING):
        a_wait(d)
    part = ga[0]
    for i in range(1, RING):
        part = part + ga[i]
    gb[me_b] = part
    for i in range(RING - 1):
        b_copy(i).start()

    acc = lax.fori_loop(half, FAR_SLOTS, target, acc)
    mmat[0:16, :] = acc[0:16] + acc[16:32]

    for i in range(RING - 1):
        b_wait(i)
    whole = gb[0]
    for i in range(1, RING):
        whole = whole + gb[i]
    gram = jnp.concatenate([whole, jnp.zeros((LANE - 24, LANE), f32)], axis=0)
    head, tail = coefficients(gram)
    weights = jnp.dot(head, everything, precision=HIGH, preferred_element_type=f32)
    weights_ref[...] = weights[0:3]
    poly_ref[...] = pltpu.roll(tail, LANE - 12, 1)[0:3, 0:4]
    both = head + pltpu.roll(tail, 12, 1)
    mapped = jnp.dot(both, mmat[...], precision=HIGH, preferred_element_type=f32)
    mapped_ref[...] = mapped[0:3]

    wait_send_all(c0, 0)
    wait_send_all(f1, 1)
    wait_send_all(f2, 2)
    for d in range(1, RING):
        a_copy(d).wait_send()
    for i in range(RING - 1):
        b_copy(i).wait_send()


def shards(source_coords, source_values, target_coords, target_owner):
    vmem = pl.BlockSpec(memory_space=pltpu.VMEM)
    dma = pltpu.SemaphoreType.DMA
    return pl.pallas_call(
        kernel,
        out_shape=(
            jax.ShapeDtypeStruct((3, OWN), f32),
            jax.ShapeDtypeStruct((3, 4), f32),
            jax.ShapeDtypeStruct((3, TGT), f32),
        ),
        in_specs=[vmem] * 4,
        out_specs=(vmem,) * 3,
        scratch_shapes=[
            pltpu.VMEM((FAR_SLOTS, 32, LANE), f32),
            pltpu.VMEM((FAR_SLOTS, 16, LANE), f32),
            pltpu.VMEM((FAR_SLOTS, 16, LANE), f32),
            pltpu.VMEM((NEAR_SLOTS * OWN, OWN), bf16),
            pltpu.VMEM((NEAR_SLOTS * OWN, OWN), bf16),
            pltpu.VMEM((OWN, TGT), bf16),
            pltpu.VMEM((OWN, TGT), bf16),
            pltpu.VMEM((CH, 3, LANE, LANE), f32),
            pltpu.VMEM((8, OWN), f32),
            pltpu.VMEM((9, 1, TGT), f32),
            pltpu.VMEM((LANE, OWN), f32),
            pltpu.VMEM((LANE, TGT), f32),
            pltpu.VMEM((RING, 24, LANE), f32),
            pltpu.VMEM((RING, 24, LANE), f32),
            dma((3, FAR_SLOTS)),
            dma((3, FAR_SLOTS)),
            dma((RING,)),
            dma((RING,)),
            dma((RING,)),
            dma((RING,)),
        ],
        compiler_params=pltpu.CompilerParams(
            collective_id=0, has_side_effects=True, vmem_limit_bytes=62 * 1024 * 1024
        ),
    )(source_coords, source_values, target_coords, target_owner.reshape(1, TGT))


def solution(mesh):
    both = ("blk", "grp")
    return jax.shard_map(
        shards,
        mesh=mesh,
        in_specs=(P(None, both), P(None, both), P(None, both), P(both)),
        out_specs=(P(None, both), P(), P(None, both)),
        check_vma=False,
    )
```

```python
import functools
import math

import jax
import jax.numpy as jnp
from jax import lax
from jax.experimental import pallas as pl
from jax.experimental.pallas import tpu as pltpu
from jax.sharding import PartitionSpec as P

MESH = pl.DeviceIdType.MESH
ITERS = 3
REACH = 2
FAR = REACH + 1
NB = 64
NG = 4
RING = 16
OWN = 640
TGT = 512
LANE = 128
CH = OWN // LANE
SLAB = OWN * NG
NSRC = SLAB * NB
STRETCH = 4.0 * SLAB
SHIFT = 2.0
TINY = 1e-6
LOG2E = 1.4426950408889634
XSCALE = math.sqrt(0.6 * LOG2E)
GRID = math.sqrt(STRETCH * LOG2E / 4.0)
TERMS = 48
ROOT = 1.0 / math.sqrt(NSRC)
NEAR_SLOTS = (2 * REACH + 1) * NG
FAR_SLOTS = (2 * FAR + 1) * NG
MAGIC = 49152.0
KEEP = 14
f32 = jnp.float32
bf16 = jnp.bfloat16
HIGH = lax.Precision.HIGHEST


def split(v):
    hi = v.astype(bf16)
    return hi, (v - hi.astype(f32)).astype(bf16)


def least_squares(hessenberg, beta):
    count = len(hessenberg)
    right_side = [beta] + [jnp.zeros_like(beta) for k in range(count)]
    upper = []
    cosines = []
    sines = []
    for k in range(count):
        column = list(hessenberg[k])
        for i in range(k):
            top = cosines[i] * column[i] + sines[i] * column[i + 1]
            lower = -sines[i] * column[i] + cosines[i] * column[i + 1]
            column[i] = top
            column[i + 1] = lower
        radius = jnp.sqrt(column[k] * column[k] + column[k + 1] * column[k + 1])
        cosine = column[k] / radius
        sine = column[k + 1] / radius
        column[k] = radius
        cosines.append(cosine)
        sines.append(sine)
        right_side[k + 1] = -sine * right_side[k]
        right_side[k] = cosine * right_side[k]
        upper.append(column[: k + 1])
    solved = [None] * count
    for k in reversed(range(count)):
        running = right_side[k]
        for j in range(k + 1, count):
            running = running - upper[j][k] * solved[j]
        solved[k] = running / upper[k][k]
    return solved


def pieces(v, count):
    out = []
    for i in range(count):
        part = v.astype(bf16).astype(f32)
        out.append(part)
        v = v - part
    return out


def point_terms(x, y, z, column, extra):
    one = jnp.ones_like(x)
    big = 1.0 if column else 8.0
    fine = []
    coarse = []
    scalar = -x * x
    whole = jnp.zeros_like(x)
    for v in (y, z):
        u = (v - 0.5) * GRID
        n = jnp.floor(u + 0.5)
        f = u - n
        f1, f2, f3 = pieces(f, 3)
        if column:
            fine += [f1, f2, f3, n, n, n, f1, f1, f2, f2]
        else:
            n8 = 8.0 * n
            fine += [n8, n8, n8, 8.0 * f1, 8.0 * f2, 8.0 * f3, 8.0 * f1, 8.0 * f2, 8.0 * f1, 8.0 * f2]
        coarse.append(n * big)
        scalar = scalar - (8.0 * n + 4.0 * f) * f
        whole = whole - 4.0 * n * n
    s = pieces(scalar, 3)
    w = pieces(whole, 2)
    x1, x2, x3 = pieces(x, 3)
    if column:
        fine += s + [one, one, one] + [x1, x1, x2, x2, x1, x3]
        coarse += w + [one, one, one]
    else:
        fine += [one, one, one] + s + [2.0 * v for v in (x1, x2, x1, x2, x3, x1)]
        coarse += [one, one] + w + [extra]
    return fine + coarse


def basis_rows(x, y, z):
    return (
        jnp.full_like(x, ROOT),
        (2.0 * x / NB - 1.0) * ROOT,
        (2.0 * y - 1.0) * ROOT,
        (2.0 * z - 1.0) * ROOT,
    )


def coefficients(gram):
    lane = lax.broadcasted_iota(jnp.int32, (8, LANE), 1)
    row = lax.broadcasted_iota(jnp.int32, (8, LANE), 0)
    tail_lanes = (lane >= 12) & (lane < 16)

    def total(v):
        return jnp.sum(v, axis=1, keepdims=True)

    def times_gram(v):
        return jnp.dot(v, gram, precision=HIGH, preferred_element_type=f32)

    def shifted(v):
        up = pltpu.roll(v, 3, 1)
        across = pltpu.roll(v, 4, 1)
        moved = jnp.where(lane < 12, up, jnp.where((lane >= 16) & (lane < 20), across, 0.0))
        moved = jnp.where(lane < 3, 0.0, moved)
        return moved + SHIFT * v

    first = jnp.where((lane == row) & (row < 3), 1.0, 0.0)
    first_gram = times_gram(first)
    beta = jnp.sqrt(total(first_gram * first) + TINY)
    heads = [first / beta]
    tails = [jnp.zeros_like(first)]
    grams = [first_gram / beta]
    hessenberg = []
    for k in range(ITERS):
        head = shifted(heads[k]) + tails[k]
        tail = jnp.where(tail_lanes, grams[k], 0.0)
        head_gram = times_gram(head)
        column = [
            total(head_gram * heads[i]) + total(tail * tails[i]) for i in range(k + 1)
        ]
        for i in range(k + 1):
            head = head - column[i] * heads[i]
            tail = tail - column[i] * tails[i]
        rest_gram = times_gram(head)
        length = jnp.sqrt(total(rest_gram * head) + total(tail * tail) + TINY)
        column.append(length)
        hessenberg.append(column)
        heads.append(head / length)
        tails.append(tail / length)
        grams.append(rest_gram / length)
    solved = least_squares(hessenberg, beta)
    head = solved[0] * heads[0]
    tail = solved[0] * tails[0]
    for k in range(1, ITERS):
        head = head + solved[k] * heads[k]
        tail = tail + solved[k] * tails[k]
    return head, tail


def kernel(
    coords_ref,
    values_ref,
    tcoords_ref,
    owner_ref,
    weights_ref,
    poly_ref,
    mapped_ref,
    c0,
    f1,
    f2,
    kh,
    kl,
    th,
    tl,
    acc_near,
    acc_far,
    lt,
    stage,
    rsrc,
    rtgt,
    fmat,
    mmat,
    ga,
    gb,
    send_sem,
    recv_sem,
    a_send,
    a_recv,
    b_send,
    b_recv,
):
    p = lax.axis_index("blk")
    g = lax.axis_index("grp")
    xi = p // RING
    zi = p % RING
    own = FAR * NG + g

    def valid(o):
        return (p + o >= 0) & (p + o < NB)

    halo = []
    for d in range(1, NG):
        halo.append((0, (g + d) % NG))
    for dist in range(1, FAR + 1):
        for o in (dist, -dist):
            for d in range(NG):
                halo.append((o, (g + d) % NG))
    ring_a = [(xi * RING + (zi + d) % RING, g) for d in range(1, RING)]
    ring_b = [
        (((xi + dx) % 4) * RING + zi, (g + dg) % NG)
        for dx in range(4)
        for dg in range(NG)
        if (dx, dg) != (0, 0)
    ]

    barrier = pltpu.get_barrier_semaphore()

    def signal(q, h):
        pl.semaphore_signal(barrier, inc=1, device_id=(q, h), device_id_type=MESH)

    expected = NG - 1 + len(ring_a) + len(ring_b)
    for o, h in halo:
        if o == 0:
            signal(p, h)
        else:
            pl.when(valid(o))(functools.partial(signal, p + o, h))
    for o in range(-FAR, FAR + 1):
        if o != 0:
            expected = expected + jnp.where(valid(o), NG, 0)
    for q, h in ring_a + ring_b:
        signal(q, h)

    for t in range(CH):
        lanes = slice(t * LANE, (t + 1) * LANE)
        c0[own, 3 * t : 3 * t + 3, :] = coords_ref[:, lanes]
        c0[own, 16 + 3 * t : 16 + 3 * t + 3, :] = values_ref[:, lanes]
    base = p.astype(f32)
    sx, sy, sz = coords_ref[0:1, :], coords_ref[1:2, :], coords_ref[2:3, :]
    source_terms = point_terms((sx - base) * XSCALE, sy, sz, False, jnp.zeros_like(sx))
    source_terms += [jnp.zeros_like(sx)] * (TERMS - len(source_terms))
    rsrc[...] = jnp.concatenate(source_terms, axis=0).astype(bf16)
    stage[...] = jnp.zeros_like(stage)
    fmat[...] = jnp.zeros_like(fmat)
    mmat[...] = jnp.zeros_like(mmat)
    fmat[0:3, :] = values_ref[...]
    for i, part in enumerate(basis_rows(sx, sy, sz)):
        fmat[12 + i : 13 + i, :] = part
    tx, ty, tz = tcoords_ref[0:1, :], tcoords_ref[1:2, :], tcoords_ref[2:3, :]
    owner = owner_ref[...]
    target_terms = point_terms((tx - base) * XSCALE, ty, tz, False, jnp.zeros_like(tx))
    masked = len(target_terms) - 1
    target_terms += [jnp.zeros_like(tx)] * (TERMS - len(target_terms))
    target_terms = jnp.concatenate(target_terms, axis=0)
    at_mask = lax.broadcasted_iota(jnp.int32, (TERMS, TGT), 0) == masked
    for o in range(-FAR, FAR + 1):
        mask = jnp.where(jnp.abs(owner - (p + o)) <= REACH, 0.0, -1e6)
        rtgt[FAR + o] = jnp.where(at_mask, mask, target_terms).astype(bf16)
    for i, part in enumerate(basis_rows(tx, ty, tz)):
        mmat[24 + i : 25 + i, :] = part

    absent = jnp.where(
        lax.broadcasted_iota(jnp.int32, (32, LANE), 0) % 3 == 0, 1e5, 0.0
    )
    absent = jnp.where(lax.broadcasted_iota(jnp.int32, (32, LANE), 0) < 15, absent, 0.0)
    for o in range(-FAR, FAR + 1):
        if o != 0:

            @pl.when(jnp.logical_not(valid(o)))
            def _():
                for h in range(NG):
                    slot = (FAR + o) * NG + h
                    c0[slot] = absent
                    f1[slot] = jnp.zeros((16, LANE), f32)
                    f2[slot] = jnp.zeros((16, LANE), f32)

    pl.semaphore_wait(barrier, expected)

    def block_copy(buf, which, o, h):
        return pltpu.make_async_remote_copy(
            src_ref=buf.at[own],
            dst_ref=buf.at[(FAR - o) * NG + g],
            send_sem=send_sem.at[which, (FAR + o) * NG + h],
            recv_sem=recv_sem.at[which, (FAR - o) * NG + g],
            device_id=(p + o, h),
            device_id_type=MESH,
        )

    def send_all(buf, which):
        for o, h in halo:
            copy = block_copy(buf, which, o, h)
            if o == 0:
                copy.start()
            else:
                pl.when(valid(o))(copy.start)

    def wait_send_all(buf, which):
        for o, h in halo:
            copy = block_copy(buf, which, o, h)
            if o == 0:
                copy.wait_send()
            else:
                pl.when(valid(o))(copy.wait_send)

    def wait_block(buf, which, o, h):
        slot = (FAR + o) * NG + h
        pltpu.make_async_remote_copy(
            src_ref=buf.at[own],
            dst_ref=buf.at[slot],
            send_sem=send_sem.at[which, slot],
            recv_sem=recv_sem.at[which, slot],
            device_id=(p + o, h),
            device_id_type=MESH,
        ).wait_recv()

    def place(k):
        oi = lax.div(k, NG)
        dist = lax.div(oi + 1, 2)
        o = jnp.where(lax.rem(oi, 2) == 1, dist, -dist)
        h = lax.rem(g + k, NG)
        return o, h, (FAR + o) * NG + h

    send_all(c0, 0)

    def column_terms(slot, k):
        x, y, z = (c0[slot, pl.ds(i, CH, stride=3), :] for i in range(3))
        for i, v in enumerate(point_terms((x - base) * XSCALE, y, z, True, None)):
            stage[pl.ds(i, CH, stride=TERMS), :] = v
        for t in range(CH):
            at = pl.ds(pl.multiple_of(k * OWN, OWN) + t * LANE, LANE)
            lt[at, :] = stage[t * TERMS : (t + 1) * TERMS, :].T.astype(bf16)

    def fill(k, t, right, hi_ref, lo_ref, start):
        at = pl.ds(pl.multiple_of(k * OWN, OWN) + t * LANE, LANE)
        put = pl.ds(start + t * LANE, LANE)
        e = jnp.exp2(jnp.dot(lt[at, :], right, preferred_element_type=f32))
        hi = (e + MAGIC) - MAGIC
        hi_ref[put, :] = hi.astype(bf16)
        lo_ref[put, :] = (e - hi).astype(bf16)

    def near_values(slot, t):
        cc = c0[slot, 3 * t : 3 * t + 3, :]
        parts = [c0[slot, 16 + 3 * t : 16 + 3 * t + 3, :]]
        parts += basis_rows(cc[0:1], cc[1:2], cc[2:3])
        parts.append(jnp.zeros((1, LANE), f32))
        return jnp.concatenate(split(jnp.concatenate(parts, axis=0)), axis=0)

    def next_block(k, last):
        later = jnp.minimum(k + 1, last)
        o, h, slot = place(later)

        @pl.when((k < last) & valid(o))
        def _():
            wait_block(c0, 0, o, h)

        return slot

    def build(k, carry):
        slot = place(k)[2]
        upcoming = next_block(k, NEAR_SLOTS - 1)
        start = pl.multiple_of(k * OWN, OWN)

        def multiply(t):
            v = near_values(slot, t)
            at = pl.ds(start + t * LANE, LANE)
            acc_near[...] += jnp.dot(v, kh[at, :], preferred_element_type=f32) + jnp.dot(
                v, kl[at, :], preferred_element_type=f32
            )

        for t in range(CH):
            fill(k, t, rsrc[...], kh, kl, start)
            if t == 0:
                column_terms(upcoming, k + 1)
            if t > 0:
                multiply(t - 1)
        multiply(CH - 1)
        return carry

    column_terms(own, 0)
    acc_near[...] = jnp.zeros_like(acc_near)
    lax.fori_loop(0, NEAR_SLOTS, build, 0)
    acc = acc_near[...]
    image = acc[0:8] + acc[8:16]
    first = image[0:3] - SHIFT * fmat[0:3, :]
    fmat[3:6, :] = first
    fmat[16:20, :] = image[3:7] - SHIFT * fmat[12:16, :]

    def keep_own(buf, v):
        for t in range(CH):
            buf[own, 3 * t : 3 * t + 3, :] = v[:, t * LANE : (t + 1) * LANE]

    keep_own(f1, first)
    send_all(f1, 1)

    def far_values(slot, t):
        cc = c0[slot, 3 * t : 3 * t + 3, :]
        parts = [
            c0[slot, 16 + 3 * t : 16 + 3 * t + 3, :],
            f1[slot, 3 * t : 3 * t + 3, :],
            f2[slot, 3 * t : 3 * t + 3, :],
            jnp.zeros((3, LANE), f32),
        ]
        parts += basis_rows(cc[0:1], cc[1:2], cc[2:3])
        return jnp.concatenate(split(jnp.concatenate(parts, axis=0)), axis=0)

    def target_fill(k, region, after):
        o = place(k)[0]
        start = pl.multiple_of(region * OWN, OWN)
        for t in range(CH):
            fill(k, t, rtgt[FAR + o], th, tl, start)
            after(t, start)

    def target_keep(k, carry):
        target_fill(k, k, lambda t, start: None)
        return carry

    def target_multiply(slot, t, start):
        v = far_values(slot, t)
        at = pl.ds(start + t * LANE, LANE)
        acc_far[...] += jnp.dot(v, th[at, :], preferred_element_type=f32) + jnp.dot(
            v, tl[at, :], preferred_element_type=f32
        )

    def target_now(k, carry):
        o, h, slot = place(k)

        @pl.when((k >= NEAR_SLOTS) & valid(o))
        def _():
            wait_block(c0, 0, o, h)
            wait_block(f1, 1, o, h)
            wait_block(f2, 2, o, h)

        @pl.when(k >= NEAR_SLOTS)
        def _():
            column_terms(slot, k)

        def after(t, start):
            if t > 0:
                target_multiply(slot, t - 1, start)

        target_fill(k, KEEP, after)
        target_multiply(slot, CH - 1, pl.multiple_of(KEEP * OWN, OWN))
        return carry

    def target_kept(k, carry):
        slot = place(k)[2]
        start = pl.multiple_of(k * OWN, OWN)
        v = jnp.concatenate([far_values(slot, t) for t in range(CH)], axis=1)
        at = pl.ds(start, OWN)
        acc_far[...] += jnp.dot(v, th[at, :], preferred_element_type=f32) + jnp.dot(
            v, tl[at, :], preferred_element_type=f32
        )
        return carry

    def padded_split(v):
        v = jnp.concatenate([v, jnp.zeros((5, LANE), f32)], axis=0)
        return jnp.concatenate(split(v), axis=0)

    def apply_near(buf, which):
        def step(k, acc):
            o, h, slot = place(k)

            @pl.when((k > 0) & valid(o))
            def _():
                wait_block(buf, which, o, h)

            start = pl.multiple_of(k * OWN, OWN)
            v = jnp.concatenate(
                [padded_split(buf[slot, 3 * t : 3 * t + 3, :]) for t in range(CH)], axis=1
            )
            at = pl.ds(start, OWN)
            acc = acc + jnp.dot(v, kh[at, :], preferred_element_type=f32)
            return acc + jnp.dot(v, kl[at, :], preferred_element_type=f32)

        acc = lax.fori_loop(0, NEAR_SLOTS, step, jnp.zeros((16, OWN), f32))
        return acc[0:3] + acc[8:11]

    lax.fori_loop(0, KEEP // 2, target_keep, 0)
    second = apply_near(f1, 1) - SHIFT * first
    fmat[6:9, :] = second
    keep_own(f2, second)
    send_all(f2, 2)
    lax.fori_loop(KEEP // 2, KEEP, target_keep, 0)
    third = apply_near(f2, 2) - SHIFT * second
    fmat[9:12, :] = third

    everything = fmat[...]
    local = lax.dot_general(
        fmat[0:24, :],
        everything,
        (((1,), (1,)), ((), ())),
        precision=HIGH,
        preferred_element_type=f32,
    )
    ga[zi] = local[0:8] + pltpu.roll(local[8:16], 32, 1) + pltpu.roll(local[16:24], 64, 1)

    def a_copy(d):
        q, h = ring_a[d - 1]
        return pltpu.make_async_remote_copy(
            src_ref=ga.at[zi],
            dst_ref=ga.at[zi],
            send_sem=a_send.at[d],
            recv_sem=a_recv.at[zi],
            device_id=(q, h),
            device_id_type=MESH,
        )

    def a_wait(d):
        slot = (zi + d) % RING
        pltpu.make_async_remote_copy(
            src_ref=ga.at[zi],
            dst_ref=ga.at[slot],
            send_sem=a_send.at[d],
            recv_sem=a_recv.at[slot],
            device_id=ring_a[d - 1],
            device_id_type=MESH,
        ).wait_recv()

    me_b = xi * NG + g

    def b_copy(i):
        return pltpu.make_async_remote_copy(
            src_ref=gb.at[me_b],
            dst_ref=gb.at[me_b],
            send_sem=b_send.at[i],
            recv_sem=b_recv.at[me_b],
            device_id=ring_b[i],
            device_id_type=MESH,
        )

    def b_wait(i):
        dx, dg = (i + 1) // NG, (i + 1) % NG
        slot = ((xi + dx) % 4) * NG + (g + dg) % NG
        pltpu.make_async_remote_copy(
            src_ref=gb.at[me_b],
            dst_ref=gb.at[slot],
            send_sem=b_send.at[i],
            recv_sem=b_recv.at[slot],
            device_id=ring_b[i],
            device_id_type=MESH,
        ).wait_recv()

    for d in range(1, RING):
        a_copy(d).start()

    acc_far[...] = jnp.zeros_like(acc_far)
    half = KEEP + (FAR_SLOTS - KEEP) // 2
    lax.fori_loop(KEEP, half, target_now, 0)

    for d in range(1, RING):
        a_wait(d)
    part = ga[0]
    for i in range(1, RING):
        part = part + ga[i]
    gb[me_b] = part
    for i in range(RING - 1):
        b_copy(i).start()

    lax.fori_loop(half, FAR_SLOTS, target_now, 0)
    lax.fori_loop(0, KEEP, target_kept, 0)
    mmat[0:16, :] = acc_far[0:16, :] + acc_far[16:32, :]

    for i in range(RING - 1):
        b_wait(i)
    whole = gb[0]
    for i in range(1, RING):
        whole = whole + gb[i]
    few = lax.broadcasted_iota(jnp.int32, (8, LANE), 1) < 24
    parts = [whole, pltpu.roll(whole, LANE - 32, 1), pltpu.roll(whole, LANE - 64, 1)]
    parts = [jnp.where(few, part, 0.0) for part in parts]
    gram = jnp.concatenate(parts + [jnp.zeros((LANE - 24, LANE), f32)], axis=0)
    head, tail = coefficients(gram)
    weights = jnp.dot(head, everything, precision=HIGH, preferred_element_type=f32)
    weights_ref[...] = weights[0:3]
    poly_ref[...] = pltpu.roll(tail, LANE - 12, 1)[0:3, 0:4]
    both = head + pltpu.roll(tail, 12, 1)
    mapped = jnp.dot(both, mmat[...], precision=HIGH, preferred_element_type=f32)
    mapped_ref[...] = mapped[0:3]

    wait_send_all(c0, 0)
    wait_send_all(f1, 1)
    wait_send_all(f2, 2)
    for d in range(1, RING):
        a_copy(d).wait_send()
    for i in range(RING - 1):
        b_copy(i).wait_send()


def shards(source_coords, source_values, target_coords, target_owner):
    vmem = pl.BlockSpec(memory_space=pltpu.VMEM)
    dma = pltpu.SemaphoreType.DMA
    return pl.pallas_call(
        kernel,
        out_shape=(
            jax.ShapeDtypeStruct((3, OWN), f32),
            jax.ShapeDtypeStruct((3, 4), f32),
            jax.ShapeDtypeStruct((3, TGT), f32),
        ),
        in_specs=[vmem] * 4,
        out_specs=(vmem,) * 3,
        scratch_shapes=[
            pltpu.VMEM((FAR_SLOTS, 32, LANE), f32),
            pltpu.VMEM((FAR_SLOTS, 16, LANE), f32),
            pltpu.VMEM((FAR_SLOTS, 16, LANE), f32),
            pltpu.VMEM((NEAR_SLOTS * OWN, OWN), bf16),
            pltpu.VMEM((NEAR_SLOTS * OWN, OWN), bf16),
            pltpu.VMEM(((KEEP + 1) * OWN, TGT), bf16),
            pltpu.VMEM(((KEEP + 1) * OWN, TGT), bf16),
            pltpu.VMEM((16, OWN), f32),
            pltpu.VMEM((32, TGT), f32),
            pltpu.VMEM((FAR_SLOTS * OWN, TERMS), bf16),
            pltpu.VMEM((CH * TERMS, LANE), f32),
            pltpu.VMEM((TERMS, OWN), bf16),
            pltpu.VMEM((2 * FAR + 1, TERMS, TGT), bf16),
            pltpu.VMEM((LANE, OWN), f32),
            pltpu.VMEM((LANE, TGT), f32),
            pltpu.VMEM((RING, 8, LANE), f32),
            pltpu.VMEM((RING, 8, LANE), f32),
            dma((3, FAR_SLOTS)),
            dma((3, FAR_SLOTS)),
            dma((RING,)),
            dma((RING,)),
            dma((RING,)),
            dma((RING,)),
        ],
        compiler_params=pltpu.CompilerParams(
            collective_id=0, has_side_effects=True, vmem_limit_bytes=62 * 1024 * 1024
        ),
    )(source_coords, source_values, target_coords, target_owner.reshape(1, TGT))


def solution(mesh):
    both = ("blk", "grp")
    return jax.shard_map(
        shards,
        mesh=mesh,
        in_specs=(P(None, both), P(None, both), P(None, both), P(both)),
        out_specs=(P(None, both), P(), P(None, both)),
        check_vma=False,
    )
```

```python
import functools
import math

import jax
import jax.numpy as jnp
from jax import lax
from jax.experimental import pallas as pl
from jax.experimental.pallas import tpu as pltpu
from jax.sharding import PartitionSpec as P

MESH = pl.DeviceIdType.MESH
ITERS = 3
REACH = 2
FAR = REACH + 1
NB = 64
NG = 4
RING = 16
OWN = 640
TGT = 512
LANE = 128
CH = OWN // LANE
SLAB = OWN * NG
NSRC = SLAB * NB
STRETCH = 4.0 * SLAB
SHIFT = 2.0
TINY = 1e-6
LOG2E = 1.4426950408889634
XSCALE = math.sqrt(0.6 * LOG2E)
GRID = math.sqrt(STRETCH * LOG2E / 4.0)
TERMS = 48
ROOT = 1.0 / math.sqrt(NSRC)
NEAR_SLOTS = (2 * REACH + 1) * NG
FAR_SLOTS = (2 * FAR + 1) * NG
KEEP = 16
f32 = jnp.float32
bf16 = jnp.bfloat16
HIGH = lax.Precision.HIGHEST


def split(v):
    hi = v.astype(bf16)
    return hi, (v - hi.astype(f32)).astype(bf16)


def least_squares(hessenberg, beta):
    count = len(hessenberg)
    right_side = [beta] + [jnp.zeros_like(beta) for k in range(count)]
    upper = []
    cosines = []
    sines = []
    for k in range(count):
        column = list(hessenberg[k])
        for i in range(k):
            top = cosines[i] * column[i] + sines[i] * column[i + 1]
            lower = -sines[i] * column[i] + cosines[i] * column[i + 1]
            column[i] = top
            column[i + 1] = lower
        radius = jnp.sqrt(column[k] * column[k] + column[k + 1] * column[k + 1])
        cosine = column[k] / radius
        sine = column[k + 1] / radius
        column[k] = radius
        cosines.append(cosine)
        sines.append(sine)
        right_side[k + 1] = -sine * right_side[k]
        right_side[k] = cosine * right_side[k]
        upper.append(column[: k + 1])
    solved = [None] * count
    for k in reversed(range(count)):
        running = right_side[k]
        for j in range(k + 1, count):
            running = running - upper[j][k] * solved[j]
        solved[k] = running / upper[k][k]
    return solved


def pieces(v, count):
    out = []
    for i in range(count):
        part = v.astype(bf16).astype(f32)
        out.append(part)
        v = v - part
    return out


def point_terms(x, y, z, column, extra):
    one = jnp.ones_like(x)
    big = 1.0 if column else 8.0
    fine = []
    coarse = []
    scalar = -x * x
    whole = jnp.zeros_like(x)
    for v in (y, z):
        u = (v - 0.5) * GRID
        n = jnp.floor(u + 0.5)
        f = u - n
        f1, f2, f3 = pieces(f, 3)
        if column:
            fine += [f1, f2, f3, n, n, n, f1, f1, f2, f2]
        else:
            n8 = 8.0 * n
            fine += [n8, n8, n8, 8.0 * f1, 8.0 * f2, 8.0 * f3, 8.0 * f1, 8.0 * f2, 8.0 * f1, 8.0 * f2]
        coarse.append(n * big)
        scalar = scalar - (8.0 * n + 4.0 * f) * f
        whole = whole - 4.0 * n * n
    s = pieces(scalar, 3)
    w = pieces(whole, 2)
    x1, x2, x3 = pieces(x, 3)
    if column:
        fine += s + [one, one, one] + [x1, x1, x2, x2, x1, x3]
        coarse += w + [one, one, one]
    else:
        fine += [one, one, one] + s + [2.0 * v for v in (x1, x2, x1, x2, x3, x1)]
        coarse += [one, one] + w + [extra]
    return fine + coarse


def basis_rows(x, y, z):
    return (
        jnp.full_like(x, ROOT),
        (2.0 * x / NB - 1.0) * ROOT,
        (2.0 * y - 1.0) * ROOT,
        (2.0 * z - 1.0) * ROOT,
    )


def coefficients(gram):
    lane = lax.broadcasted_iota(jnp.int32, (8, LANE), 1)
    row = lax.broadcasted_iota(jnp.int32, (8, LANE), 0)
    tail_lanes = (lane >= 12) & (lane < 16)

    def total(v):
        return jnp.sum(v, axis=1, keepdims=True)

    def times_gram(v):
        return jnp.dot(v, gram, precision=HIGH, preferred_element_type=f32)

    def shifted(v):
        up = pltpu.roll(v, 3, 1)
        across = pltpu.roll(v, 4, 1)
        moved = jnp.where(lane < 12, up, jnp.where((lane >= 16) & (lane < 20), across, 0.0))
        moved = jnp.where(lane < 3, 0.0, moved)
        return moved + SHIFT * v

    first = jnp.where((lane == row) & (row < 3), 1.0, 0.0)
    first_gram = times_gram(first)
    beta = jnp.sqrt(total(first_gram * first) + TINY)
    heads = [first / beta]
    tails = [jnp.zeros_like(first)]
    grams = [first_gram / beta]
    hessenberg = []
    for k in range(ITERS):
        head = shifted(heads[k]) + tails[k]
        tail = jnp.where(tail_lanes, grams[k], 0.0)
        head_gram = times_gram(head)
        column = [
            total(head_gram * heads[i]) + total(tail * tails[i]) for i in range(k + 1)
        ]
        for i in range(k + 1):
            head = head - column[i] * heads[i]
            tail = tail - column[i] * tails[i]
        rest_gram = head_gram
        for i in range(k + 1):
            rest_gram = rest_gram - column[i] * grams[i]
        length = jnp.sqrt(total(rest_gram * head) + total(tail * tail) + TINY)
        column.append(length)
        hessenberg.append(column)
        heads.append(head / length)
        tails.append(tail / length)
        grams.append(rest_gram / length)
    solved = least_squares(hessenberg, beta)
    head = solved[0] * heads[0]
    tail = solved[0] * tails[0]
    for k in range(1, ITERS):
        head = head + solved[k] * heads[k]
        tail = tail + solved[k] * tails[k]
    return head, tail


def kernel(
    coords_ref,
    values_ref,
    tcoords_ref,
    owner_ref,
    weights_ref,
    poly_ref,
    mapped_ref,
    c0,
    f1,
    f2,
    kh,
    kl,
    th,
    tl,
    acc_near,
    acc_far,
    lt,
    stage,
    rsrc,
    rtgt,
    fmat,
    mmat,
    ga,
    gb,
    send_sem,
    recv_sem,
    a_send,
    a_recv,
    b_send,
    b_recv,
):
    p = lax.axis_index("blk")
    g = lax.axis_index("grp")
    xi = p // RING
    zi = p % RING
    own = FAR * NG + g

    def valid(o):
        return (p + o >= 0) & (p + o < NB)

    halo = []
    for d in range(1, NG):
        halo.append((0, (g + d) % NG))
    for dist in range(1, FAR + 1):
        for o in (dist, -dist):
            for d in range(NG):
                halo.append((o, (g + d) % NG))
    ring_a = [(xi * RING + (zi + d) % RING, g) for d in range(1, RING)]
    ring_b = [
        (((xi + dx) % 4) * RING + zi, (g + dg) % NG)
        for dx in range(4)
        for dg in range(NG)
        if (dx, dg) != (0, 0)
    ]

    barrier = pltpu.get_barrier_semaphore()

    def signal(q, h):
        pl.semaphore_signal(barrier, inc=1, device_id=(q, h), device_id_type=MESH)

    expected = NG - 1 + len(ring_a) + len(ring_b)
    for o, h in halo:
        if o == 0:
            signal(p, h)
        else:
            pl.when(valid(o))(functools.partial(signal, p + o, h))
    for o in range(-FAR, FAR + 1):
        if o != 0:
            expected = expected + jnp.where(valid(o), NG, 0)
    for q, h in ring_a + ring_b:
        signal(q, h)

    for t in range(CH):
        lanes = slice(t * LANE, (t + 1) * LANE)
        c0[own, 3 * t : 3 * t + 3, :] = coords_ref[:, lanes]
        c0[own, 16 + 3 * t : 16 + 3 * t + 3, :] = values_ref[:, lanes]
    base = p.astype(f32)
    sx, sy, sz = coords_ref[0:1, :], coords_ref[1:2, :], coords_ref[2:3, :]
    source_terms = point_terms((sx - base) * XSCALE, sy, sz, False, jnp.zeros_like(sx))
    source_terms += [jnp.zeros_like(sx)] * (TERMS - len(source_terms))
    rsrc[...] = jnp.concatenate(source_terms, axis=0).astype(bf16)
    stage[...] = jnp.zeros_like(stage)
    fmat[...] = jnp.zeros_like(fmat)
    mmat[...] = jnp.zeros_like(mmat)
    fmat[0:3, :] = values_ref[...]
    for i, part in enumerate(basis_rows(sx, sy, sz)):
        fmat[12 + i : 13 + i, :] = part
    tx, ty, tz = tcoords_ref[0:1, :], tcoords_ref[1:2, :], tcoords_ref[2:3, :]
    owner = owner_ref[...]
    target_terms = point_terms((tx - base) * XSCALE, ty, tz, False, jnp.zeros_like(tx))
    masked = len(target_terms) - 1
    target_terms += [jnp.zeros_like(tx)] * (TERMS - len(target_terms))
    target_terms = jnp.concatenate(target_terms, axis=0)
    at_mask = lax.broadcasted_iota(jnp.int32, (TERMS, TGT), 0) == masked
    for o in range(-FAR, FAR + 1):
        mask = jnp.where(jnp.abs(owner - (p + o)) <= REACH, 0.0, -1e6)
        rtgt[FAR + o] = jnp.where(at_mask, mask, target_terms).astype(bf16)
    for i, part in enumerate(basis_rows(tx, ty, tz)):
        mmat[24 + i : 25 + i, :] = part

    absent = jnp.where(
        lax.broadcasted_iota(jnp.int32, (32, LANE), 0) % 3 == 0, 1e5, 0.0
    )
    absent = jnp.where(lax.broadcasted_iota(jnp.int32, (32, LANE), 0) < 15, absent, 0.0)
    for o in range(-FAR, FAR + 1):
        if o != 0:

            @pl.when(jnp.logical_not(valid(o)))
            def _():
                for h in range(NG):
                    slot = (FAR + o) * NG + h
                    c0[slot] = absent
                    f1[slot] = jnp.zeros((16, LANE), f32)
                    f2[slot] = jnp.zeros((16, LANE), f32)

    pl.semaphore_wait(barrier, expected)

    def block_copy(buf, which, o, h):
        return pltpu.make_async_remote_copy(
            src_ref=buf.at[own],
            dst_ref=buf.at[(FAR - o) * NG + g],
            send_sem=send_sem.at[which, (FAR + o) * NG + h],
            recv_sem=recv_sem.at[which, (FAR - o) * NG + g],
            device_id=(p + o, h),
            device_id_type=MESH,
        )

    def send_all(buf, which):
        for o, h in halo:
            copy = block_copy(buf, which, o, h)
            if o == 0:
                copy.start()
            else:
                pl.when(valid(o))(copy.start)

    def wait_send_all(buf, which):
        for o, h in halo:
            copy = block_copy(buf, which, o, h)
            if o == 0:
                copy.wait_send()
            else:
                pl.when(valid(o))(copy.wait_send)

    def wait_block(buf, which, o, h):
        slot = (FAR + o) * NG + h
        pltpu.make_async_remote_copy(
            src_ref=buf.at[own],
            dst_ref=buf.at[slot],
            send_sem=send_sem.at[which, slot],
            recv_sem=recv_sem.at[which, slot],
            device_id=(p + o, h),
            device_id_type=MESH,
        ).wait_recv()

    def place(k):
        oi = lax.div(k, NG)
        dist = lax.div(oi + 1, 2)
        o = jnp.where(lax.rem(oi, 2) == 1, dist, -dist)
        h = lax.rem(g + k, NG)
        return o, h, (FAR + o) * NG + h

    send_all(c0, 0)

    def column_terms(slot, k):
        x, y, z = (c0[slot, pl.ds(i, CH, stride=3), :] for i in range(3))
        for i, v in enumerate(point_terms((x - base) * XSCALE, y, z, True, None)):
            stage[pl.ds(i, CH, stride=TERMS), :] = v
        for t in range(CH):
            at = pl.ds(pl.multiple_of(k * OWN, OWN) + t * LANE, LANE)
            lt[at, :] = stage[t * TERMS : (t + 1) * TERMS, :].T.astype(bf16)

    def fill(k, t, right, hi_ref, lo_ref, start):
        at = pl.ds(pl.multiple_of(k * OWN, OWN) + t * LANE, LANE)
        put = pl.ds(start + t * LANE, LANE)
        e = jnp.exp2(jnp.dot(lt[at, :], right, preferred_element_type=f32))
        hi_ref[put, :], lo_ref[put, :] = split(e)

    def near_values(slot, t):
        cc = c0[slot, 3 * t : 3 * t + 3, :]
        parts = [c0[slot, 16 + 3 * t : 16 + 3 * t + 3, :]]
        parts += basis_rows(cc[0:1], cc[1:2], cc[2:3])
        parts.append(jnp.zeros((1, LANE), f32))
        return jnp.concatenate(split(jnp.concatenate(parts, axis=0)), axis=0)

    def next_block(k, last):
        later = jnp.minimum(k + 1, last)
        o, h, slot = place(later)

        @pl.when((k < last) & valid(o))
        def _():
            wait_block(c0, 0, o, h)

        return slot

    def build(k, carry):
        upcoming = next_block(k, NEAR_SLOTS - 1)
        start = pl.multiple_of(k * OWN, OWN)

        for t in range(CH):
            fill(k, t, rsrc[...], kh, kl, start)
            if t == 0:
                column_terms(upcoming, k + 1)
        return carry

    column_terms(own, 0)
    lax.fori_loop(0, NEAR_SLOTS, build, 0)

    def blocks(m):
        return place(m * NG)[0], [place(m * NG + i)[2] for i in range(NG)]

    def product(hi_ref, lo_ref, region, values):
        v = jnp.concatenate(values, axis=1)
        at = pl.ds(pl.multiple_of(region * SLAB, SLAB), SLAB)
        return jnp.dot(v, hi_ref[at, :], preferred_element_type=f32) + jnp.dot(
            v, lo_ref[at, :], preferred_element_type=f32
        )

    def apply_first(m, carry):
        slots = blocks(m)[1]
        acc_near[...] += product(
            kh, kl, m, [near_values(slot, t) for slot in slots for t in range(CH)]
        )
        return carry

    acc_near[...] = jnp.zeros_like(acc_near)
    lax.fori_loop(0, 2 * REACH + 1, apply_first, 0)
    acc = acc_near[...]
    image = acc[0:8] + acc[8:16]
    first = image[0:3] - SHIFT * fmat[0:3, :]
    fmat[3:6, :] = first
    fmat[16:20, :] = image[3:7] - SHIFT * fmat[12:16, :]

    def keep_own(buf, v):
        for t in range(CH):
            buf[own, 3 * t : 3 * t + 3, :] = v[:, t * LANE : (t + 1) * LANE]

    keep_own(f1, first)
    send_all(f1, 1)

    def far_values(slot, t):
        cc = c0[slot, 3 * t : 3 * t + 3, :]
        parts = [
            c0[slot, 16 + 3 * t : 16 + 3 * t + 3, :],
            f1[slot, 3 * t : 3 * t + 3, :],
            f2[slot, 3 * t : 3 * t + 3, :],
            jnp.zeros((3, LANE), f32),
        ]
        parts += basis_rows(cc[0:1], cc[1:2], cc[2:3])
        return jnp.concatenate(split(jnp.concatenate(parts, axis=0)), axis=0)

    def target_build(first):
        def step(k, carry):
            o = place(k)[0]
            start = pl.multiple_of((k - first) * OWN, OWN)
            for t in range(CH):
                fill(k, t, rtgt[FAR + o], th, tl, start)
            return carry

        return step

    def target_apply(first):
        def step(m, carry):
            slots = blocks(m)[1]
            acc_far[...] += product(
                th,
                tl,
                m - first,
                [far_values(slot, t) for slot in slots for t in range(CH)],
            )
            return carry

        return step

    def last_terms(k, carry):
        o, h, slot = place(k)

        @pl.when(valid(o))
        def _():
            wait_block(c0, 0, o, h)

        column_terms(slot, k)
        return carry

    def padded_split(v):
        v = jnp.concatenate([v, jnp.zeros((5, LANE), f32)], axis=0)
        return jnp.concatenate(split(v), axis=0)

    def apply_near(buf, which):
        def step(m, carry):
            o, slots = blocks(m)
            for i in range(NG):
                h = place(m * NG + i)[1]

                @pl.when((m * NG + i > 0) & valid(o))
                def _():
                    wait_block(buf, which, o, h)

            acc_near[...] += product(
                kh,
                kl,
                m,
                [
                    padded_split(buf[slot, 3 * t : 3 * t + 3, :])
                    for slot in slots
                    for t in range(CH)
                ],
            )
            return carry

        acc_near[...] = jnp.zeros_like(acc_near)
        lax.fori_loop(0, 2 * REACH + 1, step, 0)
        return acc_near[0:3, :] + acc_near[8:11, :]

    lax.fori_loop(NEAR_SLOTS, FAR_SLOTS, last_terms, 0)
    lax.fori_loop(0, KEEP // 2, target_build(0), 0)
    second = apply_near(f1, 1) - SHIFT * first
    fmat[6:9, :] = second
    keep_own(f2, second)
    send_all(f2, 2)
    lax.fori_loop(KEEP // 2, KEEP, target_build(0), 0)
    third = apply_near(f2, 2) - SHIFT * second
    fmat[9:12, :] = third

    everything = fmat[...]
    local = lax.dot_general(
        fmat[0:24, :],
        everything,
        (((1,), (1,)), ((), ())),
        precision=HIGH,
        preferred_element_type=f32,
    )
    ga[zi] = local[0:8] + pltpu.roll(local[8:16], 32, 1) + pltpu.roll(local[16:24], 64, 1)

    def a_copy(d):
        q, h = ring_a[d - 1]
        return pltpu.make_async_remote_copy(
            src_ref=ga.at[zi],
            dst_ref=ga.at[zi],
            send_sem=a_send.at[d],
            recv_sem=a_recv.at[zi],
            device_id=(q, h),
            device_id_type=MESH,
        )

    def a_wait(d):
        slot = (zi + d) % RING
        pltpu.make_async_remote_copy(
            src_ref=ga.at[zi],
            dst_ref=ga.at[slot],
            send_sem=a_send.at[d],
            recv_sem=a_recv.at[slot],
            device_id=ring_a[d - 1],
            device_id_type=MESH,
        ).wait_recv()

    me_b = xi * NG + g

    def b_copy(i):
        return pltpu.make_async_remote_copy(
            src_ref=gb.at[me_b],
            dst_ref=gb.at[me_b],
            send_sem=b_send.at[i],
            recv_sem=b_recv.at[me_b],
            device_id=ring_b[i],
            device_id_type=MESH,
        )

    def b_wait(i):
        dx, dg = (i + 1) // NG, (i + 1) % NG
        slot = ((xi + dx) % 4) * NG + (g + dg) % NG
        pltpu.make_async_remote_copy(
            src_ref=gb.at[me_b],
            dst_ref=gb.at[slot],
            send_sem=b_send.at[i],
            recv_sem=b_recv.at[slot],
            device_id=ring_b[i],
            device_id_type=MESH,
        ).wait_recv()

    for d in range(1, RING):
        a_copy(d).start()

    acc_far[...] = jnp.zeros_like(acc_far)
    kept = KEEP // NG
    middle = KEEP + 2 * (FAR_SLOTS - KEEP) // 3
    lax.fori_loop(0, kept, target_apply(0), 0)
    lax.fori_loop(KEEP, middle, target_build(KEEP), 0)

    for d in range(1, RING):
        a_wait(d)
    part = ga[0]
    for i in range(1, RING):
        part = part + ga[i]
    gb[me_b] = part
    for i in range(RING - 1):
        b_copy(i).start()

    lax.fori_loop(middle, FAR_SLOTS, target_build(KEEP), 0)
    for o in (FAR, -FAR):
        for h in range(NG):

            @pl.when(valid(o))
            def _():
                wait_block(f1, 1, o, h)
                wait_block(f2, 2, o, h)

    lax.fori_loop(kept, 2 * FAR + 1, target_apply(kept), 0)
    mmat[0:16, :] = acc_far[0:16, :] + acc_far[16:32, :]

    for i in range(RING - 1):
        b_wait(i)
    whole = gb[0]
    for i in range(1, RING):
        whole = whole + gb[i]
    few = lax.broadcasted_iota(jnp.int32, (8, LANE), 1) < 24
    parts = [whole, pltpu.roll(whole, LANE - 32, 1), pltpu.roll(whole, LANE - 64, 1)]
    parts = [jnp.where(few, part, 0.0) for part in parts]
    gram = jnp.concatenate(parts + [jnp.zeros((LANE - 24, LANE), f32)], axis=0)
    head, tail = coefficients(gram)
    weights = jnp.dot(head, everything, precision=HIGH, preferred_element_type=f32)
    weights_ref[...] = weights[0:3]
    poly_ref[...] = pltpu.roll(tail, LANE - 12, 1)[0:3, 0:4]
    both = head + pltpu.roll(tail, 12, 1)
    mapped = jnp.dot(both, mmat[...], precision=HIGH, preferred_element_type=f32)
    mapped_ref[...] = mapped[0:3]

    wait_send_all(c0, 0)
    wait_send_all(f1, 1)
    wait_send_all(f2, 2)
    for d in range(1, RING):
        a_copy(d).wait_send()
    for i in range(RING - 1):
        b_copy(i).wait_send()


def shards(source_coords, source_values, target_coords, target_owner):
    vmem = pl.BlockSpec(memory_space=pltpu.VMEM)
    dma = pltpu.SemaphoreType.DMA
    return pl.pallas_call(
        kernel,
        out_shape=(
            jax.ShapeDtypeStruct((3, OWN), f32),
            jax.ShapeDtypeStruct((3, 4), f32),
            jax.ShapeDtypeStruct((3, TGT), f32),
        ),
        in_specs=[vmem] * 4,
        out_specs=(vmem,) * 3,
        scratch_shapes=[
            pltpu.VMEM((FAR_SLOTS, 32, LANE), f32),
            pltpu.VMEM((FAR_SLOTS, 16, LANE), f32),
            pltpu.VMEM((FAR_SLOTS, 16, LANE), f32),
            pltpu.VMEM((NEAR_SLOTS * OWN, OWN), bf16),
            pltpu.VMEM((NEAR_SLOTS * OWN, OWN), bf16),
            pltpu.VMEM((KEEP * OWN, TGT), bf16),
            pltpu.VMEM((KEEP * OWN, TGT), bf16),
            pltpu.VMEM((16, OWN), f32),
            pltpu.VMEM((32, TGT), f32),
            pltpu.VMEM((FAR_SLOTS * OWN, TERMS), bf16),
            pltpu.VMEM((CH * TERMS, LANE), f32),
            pltpu.VMEM((TERMS, OWN), bf16),
            pltpu.VMEM((2 * FAR + 1, TERMS, TGT), bf16),
            pltpu.VMEM((LANE, OWN), f32),
            pltpu.VMEM((LANE, TGT), f32),
            pltpu.VMEM((RING, 8, LANE), f32),
            pltpu.VMEM((RING, 8, LANE), f32),
            dma((3, FAR_SLOTS)),
            dma((3, FAR_SLOTS)),
            dma((RING,)),
            dma((RING,)),
            dma((RING,)),
            dma((RING,)),
        ],
        compiler_params=pltpu.CompilerParams(
            collective_id=0, has_side_effects=True, vmem_limit_bytes=62 * 1024 * 1024
        ),
    )(source_coords, source_values, target_coords, target_owner.reshape(1, TGT))


def solution(mesh):
    both = ("blk", "grp")
    return jax.shard_map(
        shards,
        mesh=mesh,
        in_specs=(P(None, both), P(None, both), P(None, both), P(both)),
        out_specs=(P(None, both), P(), P(None, both)),
        check_vma=False,
    )
```

```python
import functools
import math

import jax
import jax.numpy as jnp
from jax import lax
from jax.experimental import pallas as pl
from jax.experimental.pallas import tpu as pltpu
from jax.sharding import PartitionSpec as P

MESH = pl.DeviceIdType.MESH
ITERS = 3
REACH = 2
FAR = REACH + 1
NB = 64
NG = 4
RING = 16
OWN = 640
TGT = 512
LANE = 128
CH = OWN // LANE
SLAB = OWN * NG
NSRC = SLAB * NB
STRETCH = 4.0 * SLAB
SHIFT = 2.0
TINY = 1e-6
LOG2E = 1.4426950408889634
XSCALE = math.sqrt(0.6 * LOG2E)
GRID = math.sqrt(STRETCH * LOG2E / 4.0)
TERMS = 48
ROOT = 1.0 / math.sqrt(NSRC)
NEAR_SLOTS = (2 * REACH + 1) * NG
FAR_SLOTS = (2 * FAR + 1) * NG
KEEP = 16
f32 = jnp.float32
bf16 = jnp.bfloat16
HIGH = lax.Precision.HIGHEST


def split(v):
    hi = v.astype(bf16)
    return hi, (v - hi.astype(f32)).astype(bf16)


def least_squares(hessenberg, beta):
    count = len(hessenberg)
    right_side = [beta] + [jnp.zeros_like(beta) for k in range(count)]
    upper = []
    cosines = []
    sines = []
    for k in range(count):
        column = list(hessenberg[k])
        for i in range(k):
            top = cosines[i] * column[i] + sines[i] * column[i + 1]
            lower = -sines[i] * column[i] + cosines[i] * column[i + 1]
            column[i] = top
            column[i + 1] = lower
        radius = jnp.sqrt(column[k] * column[k] + column[k + 1] * column[k + 1])
        cosine = column[k] / radius
        sine = column[k + 1] / radius
        column[k] = radius
        cosines.append(cosine)
        sines.append(sine)
        right_side[k + 1] = -sine * right_side[k]
        right_side[k] = cosine * right_side[k]
        upper.append(column[: k + 1])
    solved = [None] * count
    for k in reversed(range(count)):
        running = right_side[k]
        for j in range(k + 1, count):
            running = running - upper[j][k] * solved[j]
        solved[k] = running / upper[k][k]
    return solved


def pieces(v, count):
    out = []
    for i in range(count):
        part = v.astype(bf16).astype(f32)
        out.append(part)
        v = v - part
    return out


def point_terms(x, y, z, column, extra):
    one = jnp.ones_like(x)
    big = 1.0 if column else 8.0
    fine = []
    coarse = []
    scalar = -x * x
    whole = jnp.zeros_like(x)
    for v in (y, z):
        u = (v - 0.5) * GRID
        n = jnp.floor(u + 0.5)
        f = u - n
        f1, f2, f3 = pieces(f, 3)
        if column:
            fine += [f1, f2, f3, n, n, n, f1, f1, f2, f2]
        else:
            n8 = 8.0 * n
            fine += [n8, n8, n8, 8.0 * f1, 8.0 * f2, 8.0 * f3, 8.0 * f1, 8.0 * f2, 8.0 * f1, 8.0 * f2]
        coarse.append(n * big)
        scalar = scalar - (8.0 * n + 4.0 * f) * f
        whole = whole - 4.0 * n * n
    s = pieces(scalar, 3)
    w = pieces(whole, 2)
    x1, x2, x3 = pieces(x, 3)
    if column:
        fine += s + [one, one, one] + [x1, x1, x2, x2, x1, x3]
        coarse += w + [one, one, one]
    else:
        fine += [one, one, one] + s + [2.0 * v for v in (x1, x2, x1, x2, x3, x1)]
        coarse += [one, one] + w + [extra]
    return fine + coarse


def basis_rows(x, y, z):
    return (
        jnp.full_like(x, ROOT),
        (2.0 * x / NB - 1.0) * ROOT,
        (2.0 * y - 1.0) * ROOT,
        (2.0 * z - 1.0) * ROOT,
    )


def coefficients(gram):
    lane = lax.broadcasted_iota(jnp.int32, (8, LANE), 1)
    row = lax.broadcasted_iota(jnp.int32, (8, LANE), 0)
    tail_lanes = (lane >= 12) & (lane < 16)

    def total(v):
        return jnp.sum(v, axis=1, keepdims=True)

    def times_gram(v):
        return jnp.dot(v, gram, precision=HIGH, preferred_element_type=f32)

    def shifted(v):
        up = pltpu.roll(v, 3, 1)
        across = pltpu.roll(v, 4, 1)
        moved = jnp.where(lane < 12, up, jnp.where((lane >= 16) & (lane < 20), across, 0.0))
        moved = jnp.where(lane < 3, 0.0, moved)
        return moved + SHIFT * v

    first = jnp.where((lane == row) & (row < 3), 1.0, 0.0)
    first_gram = times_gram(first)
    beta = jnp.sqrt(total(first_gram * first) + TINY)
    heads = [first / beta]
    tails = [jnp.zeros_like(first)]
    grams = [first_gram / beta]
    hessenberg = []
    for k in range(ITERS):
        head = shifted(heads[k]) + tails[k]
        tail = jnp.where(tail_lanes, grams[k], 0.0)
        head_gram = times_gram(head)
        column = [
            total(head_gram * heads[i]) + total(tail * tails[i]) for i in range(k + 1)
        ]
        for i in range(k + 1):
            head = head - column[i] * heads[i]
            tail = tail - column[i] * tails[i]
        rest_gram = head_gram
        for i in range(k + 1):
            rest_gram = rest_gram - column[i] * grams[i]
        length = jnp.sqrt(total(rest_gram * head) + total(tail * tail) + TINY)
        column.append(length)
        hessenberg.append(column)
        heads.append(head / length)
        tails.append(tail / length)
        grams.append(rest_gram / length)
    solved = least_squares(hessenberg, beta)
    head = solved[0] * heads[0]
    tail = solved[0] * tails[0]
    for k in range(1, ITERS):
        head = head + solved[k] * heads[k]
        tail = tail + solved[k] * tails[k]
    return head, tail


def kernel(
    coords_ref,
    values_ref,
    tcoords_ref,
    owner_ref,
    out_ref,
    c0,
    f1,
    f2,
    kh,
    kl,
    th,
    tl,
    acc_near,
    acc_far,
    lt_even,
    lt_odd,
    stage_even,
    stage_odd,
    rsrc,
    rtgt,
    fmat,
    mmat,
    ga,
    gb,
    send_sem,
    recv_sem,
    a_send,
    a_recv,
    b_send,
    b_recv,
):
    p = lax.axis_index("blk")
    g = lax.axis_index("grp")
    xi = p // RING
    zi = p % RING
    own = FAR * NG + g

    def valid(o):
        return (p + o >= 0) & (p + o < NB)

    halo = []
    for d in range(1, NG):
        halo.append((0, (g + d) % NG))
    for dist in range(1, FAR + 1):
        for o in (dist, -dist):
            for d in range(NG):
                halo.append((o, (g + d) % NG))
    ring_a = [(xi * RING + (zi + d) % RING, g) for d in range(1, RING)]
    ring_b = [
        (((xi + dx) % 4) * RING + zi, (g + dg) % NG)
        for dx in range(4)
        for dg in range(NG)
        if (dx, dg) != (0, 0)
    ]

    barrier = pltpu.get_barrier_semaphore()

    def signal(q, h):
        pl.semaphore_signal(barrier, inc=1, device_id=(q, h), device_id_type=MESH)

    expected = NG - 1 + len(ring_a) + len(ring_b)
    for o, h in halo:
        if o == 0:
            signal(p, h)
        else:
            pl.when(valid(o))(functools.partial(signal, p + o, h))
    for o in range(-FAR, FAR + 1):
        if o != 0:
            expected = expected + jnp.where(valid(o), NG, 0)
    for q, h in ring_a + ring_b:
        signal(q, h)

    for t in range(CH):
        lanes = slice(t * LANE, (t + 1) * LANE)
        c0[own, 3 * t : 3 * t + 3, :] = coords_ref[:, lanes]
        c0[own, 16 + 3 * t : 16 + 3 * t + 3, :] = values_ref[:, lanes]
    absent = jnp.where(
        lax.broadcasted_iota(jnp.int32, (32, LANE), 0) % 3 == 0, 1e5, 0.0
    )
    absent = jnp.where(lax.broadcasted_iota(jnp.int32, (32, LANE), 0) < 15, absent, 0.0)
    for o in range(-FAR, FAR + 1):
        if o != 0:

            @pl.when(jnp.logical_not(valid(o)))
            def _():
                for h in range(NG):
                    slot = (FAR + o) * NG + h
                    c0[slot] = absent
                    f1[slot] = jnp.zeros((16, LANE), f32)
                    f2[slot] = jnp.zeros((16, LANE), f32)

    pl.semaphore_wait(barrier, expected)

    def block_copy(buf, which, o, h):
        return pltpu.make_async_remote_copy(
            src_ref=buf.at[own],
            dst_ref=buf.at[(FAR - o) * NG + g],
            send_sem=send_sem.at[which, (FAR + o) * NG + h],
            recv_sem=recv_sem.at[which, (FAR - o) * NG + g],
            device_id=(p + o, h),
            device_id_type=MESH,
        )

    def send_all(buf, which, far):
        for o, h in halo:
            if (abs(o) == FAR) != far:
                continue
            copy = block_copy(buf, which, o, h)
            if o == 0:
                copy.start()
            else:
                pl.when(valid(o))(copy.start)

    def wait_send_all(buf, which):
        for o, h in halo:
            copy = block_copy(buf, which, o, h)
            if o == 0:
                copy.wait_send()
            else:
                pl.when(valid(o))(copy.wait_send)

    def wait_block(buf, which, o, h):
        slot = (FAR + o) * NG + h
        pltpu.make_async_remote_copy(
            src_ref=buf.at[own],
            dst_ref=buf.at[slot],
            send_sem=send_sem.at[which, slot],
            recv_sem=recv_sem.at[which, slot],
            device_id=(p + o, h),
            device_id_type=MESH,
        ).wait_recv()

    def place(k):
        oi = lax.div(k, NG)
        dist = lax.div(oi + 1, 2)
        o = jnp.where(lax.rem(oi, 2) == 1, dist, -dist)
        h = lax.rem(g + k, NG)
        return o, h, (FAR + o) * NG + h

    send_all(c0, 0, False)

    base = p.astype(f32)
    sx, sy, sz = coords_ref[0:1, :], coords_ref[1:2, :], coords_ref[2:3, :]
    source_terms = point_terms((sx - base) * XSCALE, sy, sz, False, jnp.zeros_like(sx))
    source_terms += [jnp.zeros_like(sx)] * (TERMS - len(source_terms))
    rsrc[...] = jnp.concatenate(source_terms, axis=0).astype(bf16)
    for stage in (stage_even, stage_odd):
        stage[...] = jnp.zeros_like(stage)
    sides = ((lt_even, stage_even), (lt_odd, stage_odd))
    fmat[...] = jnp.zeros_like(fmat)
    mmat[...] = jnp.zeros_like(mmat)
    fmat[0:3, :] = values_ref[...]
    for i, part in enumerate(basis_rows(sx, sy, sz)):
        fmat[12 + i : 13 + i, :] = part
    tx, ty, tz = tcoords_ref[0:1, :], tcoords_ref[1:2, :], tcoords_ref[2:3, :]
    owner = owner_ref[...]
    target_terms = point_terms((tx - base) * XSCALE, ty, tz, False, jnp.zeros_like(tx))
    masked = len(target_terms) - 1
    target_terms += [jnp.zeros_like(tx)] * (TERMS - len(target_terms))
    target_terms = jnp.concatenate(target_terms, axis=0)
    at_mask = lax.broadcasted_iota(jnp.int32, (TERMS, TGT), 0) == masked
    for o in range(-FAR, FAR + 1):
        mask = jnp.where(jnp.abs(owner - (p + o)) <= REACH, 0.0, -1e6)
        rtgt[FAR + o] = jnp.where(at_mask, mask, target_terms).astype(bf16)
    for i, part in enumerate(basis_rows(tx, ty, tz)):
        mmat[24 + i : 25 + i, :] = part


    def column_terms(slot, pair, side):
        lt, stage = sides[side]
        x, y, z = (c0[slot, pl.ds(i, CH, stride=3), :] for i in range(3))
        for i, v in enumerate(point_terms((x - base) * XSCALE, y, z, True, None)):
            stage[pl.ds(i, CH, stride=TERMS), :] = v
        for t in range(CH):
            at = pl.ds(pl.multiple_of(pair * OWN, OWN) + t * LANE, LANE)
            lt[at, :] = stage[t * TERMS : (t + 1) * TERMS, :].T.astype(bf16)

    def fill(pair, side, right, hi_ref, lo_ref, start):
        for t in range(CH):
            at = pl.ds(pl.multiple_of(pair * OWN, OWN) + t * LANE, LANE)
            put = pl.ds(start + t * LANE, LANE)
            e = jnp.exp2(jnp.dot(sides[side][0][at, :], right, preferred_element_type=f32))
            hi_ref[put, :], lo_ref[put, :] = split(e)

    def near_values(slot, t):
        cc = c0[slot, 3 * t : 3 * t + 3, :]
        parts = [c0[slot, 16 + 3 * t : 16 + 3 * t + 3, :]]
        parts += basis_rows(cc[0:1], cc[1:2], cc[2:3])
        parts.append(jnp.zeros((1, LANE), f32))
        return jnp.concatenate(split(jnp.concatenate(parts, axis=0)), axis=0)

    def arrived(k, last):
        o, h, slot = place(jnp.minimum(k, last))

        @pl.when((k <= last) & valid(o))
        def _():
            wait_block(c0, 0, o, h)

        return slot

    def build(pair, carry):
        odd = arrived(2 * pair + 1, NEAR_SLOTS - 1)
        even = arrived(2 * pair + 2, NEAR_SLOTS - 1)
        start = pl.multiple_of(pair * 2 * OWN, 2 * OWN)
        column_terms(odd, pair, 1)
        fill(pair, 0, rsrc[...], kh, kl, start)
        column_terms(even, pair + 1, 0)
        fill(pair, 1, rsrc[...], kh, kl, start + OWN)
        return carry

    column_terms(own, 0, 0)
    lax.fori_loop(0, NEAR_SLOTS // 2, build, 0)

    def blocks(m):
        return place(m * NG)[0], [place(m * NG + i)[2] for i in range(NG)]

    def product(hi_ref, lo_ref, region, values):
        v = jnp.concatenate(values, axis=1)
        at = pl.ds(pl.multiple_of(region * SLAB, SLAB), SLAB)
        return jnp.dot(v, hi_ref[at, :], preferred_element_type=f32) + jnp.dot(
            v, lo_ref[at, :], preferred_element_type=f32
        )

    def apply_first(m, carry):
        slots = blocks(m)[1]
        acc_near[...] += product(
            kh, kl, m, [near_values(slot, t) for slot in slots for t in range(CH)]
        )
        return carry

    acc_near[...] = jnp.zeros_like(acc_near)
    lax.fori_loop(0, 2 * REACH + 1, apply_first, 0)
    acc = acc_near[...]
    image = acc[0:8] + acc[8:16]
    first = image[0:3] - SHIFT * fmat[0:3, :]
    fmat[3:6, :] = first
    fmat[16:20, :] = image[3:7] - SHIFT * fmat[12:16, :]

    def keep_own(buf, v):
        for t in range(CH):
            buf[own, 3 * t : 3 * t + 3, :] = v[:, t * LANE : (t + 1) * LANE]

    keep_own(f1, first)
    send_all(f1, 1, False)
    send_all(c0, 0, True)
    send_all(f1, 1, True)

    def far_values(slot, t):
        cc = c0[slot, 3 * t : 3 * t + 3, :]
        parts = [
            c0[slot, 16 + 3 * t : 16 + 3 * t + 3, :],
            f1[slot, 3 * t : 3 * t + 3, :],
            f2[slot, 3 * t : 3 * t + 3, :],
            jnp.zeros((3, LANE), f32),
        ]
        parts += basis_rows(cc[0:1], cc[1:2], cc[2:3])
        return jnp.concatenate(split(jnp.concatenate(parts, axis=0)), axis=0)

    def target_build(first):
        def step(pair, carry):
            start = pl.multiple_of((2 * pair - first) * OWN, 2 * OWN)
            right = rtgt[FAR + place(2 * pair)[0]]
            fill(pair, 0, right, th, tl, start)
            fill(pair, 1, right, th, tl, start + OWN)
            return carry

        return step

    def target_apply(first):
        def step(m, carry):
            slots = blocks(m)[1]
            acc_far[...] += product(
                th,
                tl,
                m - first,
                [far_values(slot, t) for slot in slots for t in range(CH)],
            )
            return carry

        return step

    def last_terms(pair, carry):
        even = arrived(2 * pair, FAR_SLOTS - 1)
        odd = arrived(2 * pair + 1, FAR_SLOTS - 1)
        column_terms(even, pair, 0)
        column_terms(odd, pair, 1)
        return carry

    def padded_split(v):
        v = jnp.concatenate([v, jnp.zeros((5, LANE), f32)], axis=0)
        return jnp.concatenate(split(v), axis=0)

    def apply_near(buf, which):
        def step(m, carry):
            o, slots = blocks(m)
            for i in range(NG):
                h = place(m * NG + i)[1]

                @pl.when((m * NG + i > 0) & valid(o))
                def _():
                    wait_block(buf, which, o, h)

            acc_near[...] += product(
                kh,
                kl,
                m,
                [
                    padded_split(buf[slot, 3 * t : 3 * t + 3, :])
                    for slot in slots
                    for t in range(CH)
                ],
            )
            return carry

        acc_near[...] = jnp.zeros_like(acc_near)
        lax.fori_loop(0, 2 * REACH + 1, step, 0)
        return acc_near[0:3, :] + acc_near[8:11, :]

    lax.fori_loop(0, KEEP // 4, target_build(0), 0)
    second = apply_near(f1, 1) - SHIFT * first
    fmat[6:9, :] = second
    keep_own(f2, second)
    send_all(f2, 2, False)
    send_all(f2, 2, True)
    lax.fori_loop(KEEP // 4, KEEP // 2, target_build(0), 0)
    lax.fori_loop(NEAR_SLOTS // 2, FAR_SLOTS // 2, last_terms, 0)
    third = apply_near(f2, 2) - SHIFT * second
    fmat[9:12, :] = third

    everything = fmat[...]
    local = lax.dot_general(
        fmat[0:24, :],
        everything,
        (((1,), (1,)), ((), ())),
        precision=HIGH,
        preferred_element_type=f32,
    )
    ga[zi] = local[0:8] + pltpu.roll(local[8:16], 32, 1) + pltpu.roll(local[16:24], 64, 1)

    def a_copy(d):
        q, h = ring_a[d - 1]
        return pltpu.make_async_remote_copy(
            src_ref=ga.at[zi],
            dst_ref=ga.at[zi],
            send_sem=a_send.at[d],
            recv_sem=a_recv.at[zi],
            device_id=(q, h),
            device_id_type=MESH,
        )

    def a_wait(d):
        slot = (zi + d) % RING
        pltpu.make_async_remote_copy(
            src_ref=ga.at[zi],
            dst_ref=ga.at[slot],
            send_sem=a_send.at[d],
            recv_sem=a_recv.at[slot],
            device_id=ring_a[d - 1],
            device_id_type=MESH,
        ).wait_recv()

    me_b = xi * NG + g

    def b_copy(i):
        return pltpu.make_async_remote_copy(
            src_ref=gb.at[me_b],
            dst_ref=gb.at[me_b],
            send_sem=b_send.at[i],
            recv_sem=b_recv.at[me_b],
            device_id=ring_b[i],
            device_id_type=MESH,
        )

    def b_wait(i):
        dx, dg = (i + 1) // NG, (i + 1) % NG
        slot = ((xi + dx) % 4) * NG + (g + dg) % NG
        pltpu.make_async_remote_copy(
            src_ref=gb.at[me_b],
            dst_ref=gb.at[slot],
            send_sem=b_send.at[i],
            recv_sem=b_recv.at[slot],
            device_id=ring_b[i],
            device_id_type=MESH,
        ).wait_recv()

    for d in range(1, RING):
        a_copy(d).start()

    acc_far[...] = jnp.zeros_like(acc_far)
    kept = KEEP // NG
    middle = KEEP + 2 * (FAR_SLOTS - KEEP) // 3
    lax.fori_loop(0, kept, target_apply(0), 0)
    lax.fori_loop(KEEP // 2, middle // 2, target_build(KEEP), 0)

    for d in range(1, RING):
        a_wait(d)
    part = ga[0]
    for i in range(1, RING):
        part = part + ga[i]
    gb[me_b] = part
    for i in range(RING - 1):
        b_copy(i).start()

    lax.fori_loop(middle // 2, FAR_SLOTS // 2, target_build(KEEP), 0)
    for o in (FAR, -FAR):
        for h in range(NG):

            @pl.when(valid(o))
            def _():
                wait_block(f1, 1, o, h)
                wait_block(f2, 2, o, h)

    lax.fori_loop(kept, 2 * FAR + 1, target_apply(kept), 0)
    mmat[0:16, :] = acc_far[0:16, :] + acc_far[16:32, :]

    for i in range(RING - 1):
        b_wait(i)
    whole = gb[0]
    for i in range(1, RING):
        whole = whole + gb[i]
    few = lax.broadcasted_iota(jnp.int32, (8, LANE), 1) < 24
    parts = [whole, pltpu.roll(whole, LANE - 32, 1), pltpu.roll(whole, LANE - 64, 1)]
    parts = [jnp.where(few, part, 0.0) for part in parts]
    gram = jnp.concatenate(parts + [jnp.zeros((LANE - 24, LANE), f32)], axis=0)
    head, tail = coefficients(gram)
    weights = jnp.dot(head, everything, precision=HIGH, preferred_element_type=f32)
    out_ref[:, 0:OWN] = weights
    out_ref[:, OWN + TGT :] = pltpu.roll(tail, LANE - 12, 1)
    both = head + pltpu.roll(tail, 12, 1)
    mapped = jnp.dot(both, mmat[...], precision=HIGH, preferred_element_type=f32)
    out_ref[:, OWN : OWN + TGT] = mapped

    wait_send_all(c0, 0)
    wait_send_all(f1, 1)
    wait_send_all(f2, 2)
    for d in range(1, RING):
        a_copy(d).wait_send()
    for i in range(RING - 1):
        b_copy(i).wait_send()


def unpack(packed_ref, weights_ref, poly_ref, mapped_ref):
    weights_ref[...] = packed_ref[0:3, 0:OWN]
    mapped_ref[...] = packed_ref[0:3, OWN : OWN + TGT]
    poly_ref[...] = packed_ref[0:3, OWN + TGT : OWN + TGT + 4]


def shards(source_coords, source_values, target_coords, target_owner):
    vmem = pl.BlockSpec(memory_space=pltpu.VMEM)
    dma = pltpu.SemaphoreType.DMA
    packed = pl.pallas_call(
        kernel,
        out_shape=jax.ShapeDtypeStruct((8, OWN + TGT + LANE), f32),
        in_specs=[vmem] * 4,
        out_specs=vmem,
        scratch_shapes=[
            pltpu.VMEM((FAR_SLOTS, 32, LANE), f32),
            pltpu.VMEM((FAR_SLOTS, 16, LANE), f32),
            pltpu.VMEM((FAR_SLOTS, 16, LANE), f32),
            pltpu.VMEM((NEAR_SLOTS * OWN, OWN), bf16),
            pltpu.VMEM((NEAR_SLOTS * OWN, OWN), bf16),
            pltpu.VMEM((KEEP * OWN, TGT), bf16),
            pltpu.VMEM((KEEP * OWN, TGT), bf16),
            pltpu.VMEM((16, OWN), f32),
            pltpu.VMEM((32, TGT), f32),
            pltpu.VMEM((FAR_SLOTS // 2 * OWN, TERMS), bf16),
            pltpu.VMEM((FAR_SLOTS // 2 * OWN, TERMS), bf16),
            pltpu.VMEM((CH * TERMS, LANE), f32),
            pltpu.VMEM((CH * TERMS, LANE), f32),
            pltpu.VMEM((TERMS, OWN), bf16),
            pltpu.VMEM((2 * FAR + 1, TERMS, TGT), bf16),
            pltpu.VMEM((LANE, OWN), f32),
            pltpu.VMEM((LANE, TGT), f32),
            pltpu.VMEM((RING, 8, LANE), f32),
            pltpu.VMEM((RING, 8, LANE), f32),
            dma((3, FAR_SLOTS)),
            dma((3, FAR_SLOTS)),
            dma((RING,)),
            dma((RING,)),
            dma((RING,)),
            dma((RING,)),
        ],
        compiler_params=pltpu.CompilerParams(
            collective_id=0, has_side_effects=True, vmem_limit_bytes=62 * 1024 * 1024
        ),
    )(source_coords, source_values, target_coords, target_owner.reshape(1, TGT))
    return pl.pallas_call(
        unpack,
        out_shape=(
            jax.ShapeDtypeStruct((3, OWN), f32),
            jax.ShapeDtypeStruct((3, 4), f32),
            jax.ShapeDtypeStruct((3, TGT), f32),
        ),
        in_specs=[vmem],
        out_specs=(vmem,) * 3,
    )(packed)


def solution(mesh):
    both = ("blk", "grp")
    return jax.shard_map(
        shards,
        mesh=mesh,
        in_specs=(P(None, both), P(None, both), P(None, both), P(both)),
        out_specs=(P(None, both), P(), P(None, both)),
        check_vma=False,
    )
```

```python
import functools
import math

import jax
import jax.numpy as jnp
from jax import lax
from jax.experimental import pallas as pl
from jax.experimental.pallas import tpu as pltpu
from jax.sharding import PartitionSpec as P

MESH = pl.DeviceIdType.MESH
ITERS = 3
REACH = 2
FAR = REACH + 1
NB = 64
NG = 4
RING = 16
OWN = 640
TGT = 512
LANE = 128
CH = OWN // LANE
SLAB = OWN * NG
NSRC = SLAB * NB
STRETCH = 4.0 * SLAB
SHIFT = 2.0
TINY = 1e-6
LOG2E = 1.4426950408889634
XSCALE = math.sqrt(0.6 * LOG2E)
GRID = math.sqrt(STRETCH * LOG2E / 4.0)
TERMS = 48
ROOT = 1.0 / math.sqrt(NSRC)
NEAR_SLOTS = (2 * REACH + 1) * NG
FAR_SLOTS = (2 * FAR + 1) * NG
KEEP = 16
f32 = jnp.float32
bf16 = jnp.bfloat16
HIGH = lax.Precision.HIGHEST


def split(v):
    hi = v.astype(bf16)
    return hi, (v - hi.astype(f32)).astype(bf16)


def least_squares(hessenberg, beta):
    count = len(hessenberg)
    right_side = [beta] + [jnp.zeros_like(beta) for k in range(count)]
    upper = []
    cosines = []
    sines = []
    for k in range(count):
        column = list(hessenberg[k])
        for i in range(k):
            top = cosines[i] * column[i] + sines[i] * column[i + 1]
            lower = -sines[i] * column[i] + cosines[i] * column[i + 1]
            column[i] = top
            column[i + 1] = lower
        radius = jnp.sqrt(column[k] * column[k] + column[k + 1] * column[k + 1])
        cosine = column[k] / radius
        sine = column[k + 1] / radius
        column[k] = radius
        cosines.append(cosine)
        sines.append(sine)
        right_side[k + 1] = -sine * right_side[k]
        right_side[k] = cosine * right_side[k]
        upper.append(column[: k + 1])
    solved = [None] * count
    for k in reversed(range(count)):
        running = right_side[k]
        for j in range(k + 1, count):
            running = running - upper[j][k] * solved[j]
        solved[k] = running / upper[k][k]
    return solved


def pieces(v, count):
    out = []
    for i in range(count):
        part = v.astype(bf16).astype(f32)
        out.append(part)
        v = v - part
    return out


def point_terms(x, y, z, column, extra):
    one = jnp.ones_like(x)
    big = 1.0 if column else 8.0
    fine = []
    coarse = []
    scalar = -x * x
    whole = jnp.zeros_like(x)
    for v in (y, z):
        u = (v - 0.5) * GRID
        n = jnp.floor(u + 0.5)
        f = u - n
        f1, f2, f3 = pieces(f, 3)
        if column:
            fine += [f1, f2, f3, n, n, n, f1, f1, f2, f2]
        else:
            n8 = 8.0 * n
            fine += [n8, n8, n8, 8.0 * f1, 8.0 * f2, 8.0 * f3, 8.0 * f1, 8.0 * f2, 8.0 * f1, 8.0 * f2]
        coarse.append(n * big)
        scalar = scalar - (8.0 * n + 4.0 * f) * f
        whole = whole - 4.0 * n * n
    s = pieces(scalar, 3)
    w = pieces(whole, 2)
    x1, x2, x3 = pieces(x, 3)
    if column:
        fine += s + [one, one, one] + [x1, x1, x2, x2, x1, x3]
        coarse += w + [one, one, one]
    else:
        fine += [one, one, one] + s + [2.0 * v for v in (x1, x2, x1, x2, x3, x1)]
        coarse += [one, one] + w + [extra]
    return fine + coarse


def basis_rows(x, y, z):
    return (
        jnp.full_like(x, ROOT),
        (2.0 * x / NB - 1.0) * ROOT,
        (2.0 * y - 1.0) * ROOT,
        (2.0 * z - 1.0) * ROOT,
    )


def coefficients(gram):
    lane = lax.broadcasted_iota(jnp.int32, (8, LANE), 1)
    row = lax.broadcasted_iota(jnp.int32, (8, LANE), 0)
    tail_lanes = (lane >= 12) & (lane < 16)

    def total(v):
        return jnp.sum(v, axis=1, keepdims=True)

    def times_gram(v):
        return jnp.dot(v[:, 0:24], gram, precision=HIGH, preferred_element_type=f32)

    def shifted(v):
        up = pltpu.roll(v, 3, 1)
        across = pltpu.roll(v, 4, 1)
        moved = jnp.where(lane < 12, up, jnp.where((lane >= 16) & (lane < 20), across, 0.0))
        moved = jnp.where(lane < 3, 0.0, moved)
        return moved + SHIFT * v

    first = jnp.where((lane == row) & (row < 3), 1.0, 0.0)
    first_gram = times_gram(first)
    beta = jnp.sqrt(total(first_gram * first) + TINY)
    heads = [first / beta]
    tails = [jnp.zeros_like(first)]
    grams = [first_gram / beta]
    hessenberg = []
    for k in range(ITERS):
        head = shifted(heads[k]) + tails[k]
        tail = jnp.where(tail_lanes, grams[k], 0.0)
        head_gram = times_gram(head)
        column = [
            total(head_gram * heads[i]) + total(tail * tails[i]) for i in range(k + 1)
        ]
        for i in range(k + 1):
            head = head - column[i] * heads[i]
            tail = tail - column[i] * tails[i]
        rest_gram = head_gram
        for i in range(k + 1):
            rest_gram = rest_gram - column[i] * grams[i]
        length = jnp.sqrt(total(rest_gram * head) + total(tail * tail) + TINY)
        column.append(length)
        hessenberg.append(column)
        heads.append(head / length)
        tails.append(tail / length)
        grams.append(rest_gram / length)
    solved = least_squares(hessenberg, beta)
    head = solved[0] * heads[0]
    tail = solved[0] * tails[0]
    for k in range(1, ITERS):
        head = head + solved[k] * heads[k]
        tail = tail + solved[k] * tails[k]
    return head, tail


def kernel(
    coords_ref,
    values_ref,
    tcoords_ref,
    owner_ref,
    out_ref,
    c0,
    f1,
    f2,
    kh,
    kl,
    th,
    tl,
    acc_near,
    acc_far,
    lt_even,
    lt_odd,
    stage_even,
    stage_odd,
    rsrc,
    rtgt,
    fmat,
    mmat,
    ga,
    gb,
    send_sem,
    recv_sem,
    a_send,
    a_recv,
    b_send,
    b_recv,
):
    p = lax.axis_index("blk")
    g = lax.axis_index("grp")
    xi = p // RING
    zi = p % RING
    own = FAR * NG + g

    def valid(o):
        return (p + o >= 0) & (p + o < NB)

    halo = []
    for d in range(1, NG):
        halo.append((0, (g + d) % NG))
    for dist in range(1, FAR + 1):
        for o in (dist, -dist):
            for d in range(NG):
                halo.append((o, (g + d) % NG))
    ring_a = [(xi * RING + (zi + d) % RING, g) for d in range(1, RING)]
    ring_b = [
        (((xi + dx) % 4) * RING + zi, (g + dg) % NG)
        for dx in range(4)
        for dg in range(NG)
        if (dx, dg) != (0, 0)
    ]

    barrier = pltpu.get_barrier_semaphore()

    def signal(q, h):
        pl.semaphore_signal(barrier, inc=1, device_id=(q, h), device_id_type=MESH)

    expected = NG - 1 + len(ring_a) + len(ring_b)
    for o, h in halo:
        if o == 0:
            signal(p, h)
        else:
            pl.when(valid(o))(functools.partial(signal, p + o, h))
    for o in range(-FAR, FAR + 1):
        if o != 0:
            expected = expected + jnp.where(valid(o), NG, 0)
    for q, h in ring_a + ring_b:
        signal(q, h)

    for t in range(CH):
        lanes = slice(t * LANE, (t + 1) * LANE)
        c0[own, 3 * t : 3 * t + 3, :] = coords_ref[:, lanes]
        c0[own, 16 + 3 * t : 16 + 3 * t + 3, :] = values_ref[:, lanes]
    absent = jnp.where(
        lax.broadcasted_iota(jnp.int32, (32, LANE), 0) % 3 == 0, 1e5, 0.0
    )
    absent = jnp.where(lax.broadcasted_iota(jnp.int32, (32, LANE), 0) < 15, absent, 0.0)
    for o in range(-FAR, FAR + 1):
        if o != 0:

            @pl.when(jnp.logical_not(valid(o)))
            def _():
                for h in range(NG):
                    slot = (FAR + o) * NG + h
                    c0[slot] = absent
                    f1[slot] = jnp.zeros((16, LANE), f32)
                    f2[slot] = jnp.zeros((16, LANE), f32)

    pl.semaphore_wait(barrier, expected)

    def block_copy(buf, which, o, h):
        return pltpu.make_async_remote_copy(
            src_ref=buf.at[own],
            dst_ref=buf.at[(FAR - o) * NG + g],
            send_sem=send_sem.at[which, (FAR + o) * NG + h],
            recv_sem=recv_sem.at[which, (FAR - o) * NG + g],
            device_id=(p + o, h),
            device_id_type=MESH,
        )

    def send_all(buf, which, far):
        for o, h in halo:
            if (abs(o) == FAR) != far:
                continue
            copy = block_copy(buf, which, o, h)
            if o == 0:
                copy.start()
            else:
                pl.when(valid(o))(copy.start)

    def wait_send_all(buf, which):
        for o, h in halo:
            copy = block_copy(buf, which, o, h)
            if o == 0:
                copy.wait_send()
            else:
                pl.when(valid(o))(copy.wait_send)

    def wait_block(buf, which, o, h):
        slot = (FAR + o) * NG + h
        pltpu.make_async_remote_copy(
            src_ref=buf.at[own],
            dst_ref=buf.at[slot],
            send_sem=send_sem.at[which, slot],
            recv_sem=recv_sem.at[which, slot],
            device_id=(p + o, h),
            device_id_type=MESH,
        ).wait_recv()

    def place(k):
        oi = lax.div(k, NG)
        dist = lax.div(oi + 1, 2)
        o = jnp.where(lax.rem(oi, 2) == 1, dist, -dist)
        h = lax.rem(g + k, NG)
        return o, h, (FAR + o) * NG + h

    send_all(c0, 0, False)

    base = p.astype(f32)
    sx, sy, sz = coords_ref[0:1, :], coords_ref[1:2, :], coords_ref[2:3, :]
    source_terms = point_terms((sx - base) * XSCALE, sy, sz, False, jnp.zeros_like(sx))
    source_terms += [jnp.zeros_like(sx)] * (TERMS - len(source_terms))
    rsrc[...] = jnp.concatenate(source_terms, axis=0).astype(bf16)
    for stage in (stage_even, stage_odd):
        stage[...] = jnp.zeros_like(stage)
    sides = ((lt_even, stage_even), (lt_odd, stage_odd))
    fmat[...] = jnp.zeros_like(fmat)
    mmat[...] = jnp.zeros_like(mmat)
    fmat[0:3, :] = values_ref[...]
    for i, part in enumerate(basis_rows(sx, sy, sz)):
        fmat[12 + i : 13 + i, :] = part
    tx, ty, tz = tcoords_ref[0:1, :], tcoords_ref[1:2, :], tcoords_ref[2:3, :]
    owner = owner_ref[...]
    target_terms = point_terms((tx - base) * XSCALE, ty, tz, False, jnp.zeros_like(tx))
    masked = len(target_terms) - 1
    target_terms += [jnp.zeros_like(tx)] * (TERMS - len(target_terms))
    target_terms = jnp.concatenate(target_terms, axis=0)
    at_mask = lax.broadcasted_iota(jnp.int32, (TERMS, TGT), 0) == masked
    for o in range(-FAR, FAR + 1):
        mask = jnp.where(jnp.abs(owner - (p + o)) <= REACH, 0.0, -1e6)
        rtgt[FAR + o] = jnp.where(at_mask, mask, target_terms).astype(bf16)
    for i, part in enumerate(basis_rows(tx, ty, tz)):
        mmat[24 + i : 25 + i, :] = part


    def column_terms(slot, pair, side):
        lt, stage = sides[side]
        x, y, z = (c0[slot, pl.ds(i, CH, stride=3), :] for i in range(3))
        for i, v in enumerate(point_terms((x - base) * XSCALE, y, z, True, None)):
            stage[pl.ds(i, CH, stride=TERMS), :] = v
        for t in range(CH):
            at = pl.ds(pl.multiple_of(pair * OWN, OWN) + t * LANE, LANE)
            lt[at, :] = stage[t * TERMS : (t + 1) * TERMS, :].T.astype(bf16)

    def fill(pair, side, right, hi_ref, lo_ref, start):
        for t in range(CH):
            at = pl.ds(pl.multiple_of(pair * OWN, OWN) + t * LANE, LANE)
            put = pl.ds(start + t * LANE, LANE)
            e = jnp.exp2(jnp.dot(sides[side][0][at, :], right, preferred_element_type=f32))
            hi_ref[put, :], lo_ref[put, :] = split(e)

    def near_values(slot, t):
        cc = c0[slot, 3 * t : 3 * t + 3, :]
        parts = [c0[slot, 16 + 3 * t : 16 + 3 * t + 3, :]]
        parts += basis_rows(cc[0:1], cc[1:2], cc[2:3])
        parts.append(jnp.zeros((1, LANE), f32))
        return jnp.concatenate(split(jnp.concatenate(parts, axis=0)), axis=0)

    def arrived(k, last):
        o, h, slot = place(jnp.minimum(k, last))

        @pl.when((k <= last) & valid(o))
        def _():
            wait_block(c0, 0, o, h)

        return slot

    def build(pair, carry):
        odd = arrived(2 * pair + 1, NEAR_SLOTS - 1)
        even = arrived(2 * pair + 2, NEAR_SLOTS - 1)
        start = pl.multiple_of(pair * 2 * OWN, 2 * OWN)
        column_terms(odd, pair, 1)
        fill(pair, 0, rsrc[...], kh, kl, start)
        column_terms(even, pair + 1, 0)
        fill(pair, 1, rsrc[...], kh, kl, start + OWN)
        return carry

    column_terms(own, 0, 0)
    lax.fori_loop(0, NEAR_SLOTS // 2, build, 0)

    def blocks(m):
        return place(m * NG)[0], [place(m * NG + i)[2] for i in range(NG)]

    def product(hi_ref, lo_ref, region, values):
        v = jnp.concatenate(values, axis=1)
        at = pl.ds(pl.multiple_of(region * SLAB, SLAB), SLAB)
        return jnp.dot(v, hi_ref[at, :], preferred_element_type=f32) + jnp.dot(
            v, lo_ref[at, :], preferred_element_type=f32
        )

    def apply_first(m, carry):
        slots = blocks(m)[1]
        acc_near[...] += product(
            kh, kl, m, [near_values(slot, t) for slot in slots for t in range(CH)]
        )
        return carry

    acc_near[...] = jnp.zeros_like(acc_near)
    lax.fori_loop(0, 2 * REACH + 1, apply_first, 0)
    acc = acc_near[...]
    image = acc[0:8] + acc[8:16]
    first = image[0:3] - SHIFT * fmat[0:3, :]
    fmat[3:6, :] = first
    fmat[16:20, :] = image[3:7] - SHIFT * fmat[12:16, :]

    def keep_own(buf, v):
        for t in range(CH):
            buf[own, 3 * t : 3 * t + 3, :] = v[:, t * LANE : (t + 1) * LANE]

    keep_own(f1, first)
    send_all(f1, 1, False)
    send_all(c0, 0, True)
    send_all(f1, 1, True)

    def far_values(slot, t):
        cc = c0[slot, 3 * t : 3 * t + 3, :]
        parts = [
            c0[slot, 16 + 3 * t : 16 + 3 * t + 3, :],
            f1[slot, 3 * t : 3 * t + 3, :],
            f2[slot, 3 * t : 3 * t + 3, :],
            jnp.zeros((3, LANE), f32),
        ]
        parts += basis_rows(cc[0:1], cc[1:2], cc[2:3])
        return jnp.concatenate(split(jnp.concatenate(parts, axis=0)), axis=0)

    def target_build(first):
        def step(pair, carry):
            start = pl.multiple_of((2 * pair - first) * OWN, 2 * OWN)
            right = rtgt[FAR + place(2 * pair)[0]]
            fill(pair, 0, right, th, tl, start)
            fill(pair, 1, right, th, tl, start + OWN)
            return carry

        return step

    def target_apply(first):
        def step(m, carry):
            slots = blocks(m)[1]
            acc_far[...] += product(
                th,
                tl,
                m - first,
                [far_values(slot, t) for slot in slots for t in range(CH)],
            )
            return carry

        return step

    def last_terms(pair, carry):
        even = arrived(2 * pair, FAR_SLOTS - 1)
        odd = arrived(2 * pair + 1, FAR_SLOTS - 1)
        column_terms(even, pair, 0)
        column_terms(odd, pair, 1)
        return carry

    def padded_split(v):
        v = jnp.concatenate([v, jnp.zeros((5, LANE), f32)], axis=0)
        return jnp.concatenate(split(v), axis=0)

    def apply_near(buf, which):
        def step(m, carry):
            o, slots = blocks(m)
            for i in range(NG):
                h = place(m * NG + i)[1]

                @pl.when((m * NG + i > 0) & valid(o))
                def _():
                    wait_block(buf, which, o, h)

            acc_near[...] += product(
                kh,
                kl,
                m,
                [
                    padded_split(buf[slot, 3 * t : 3 * t + 3, :])
                    for slot in slots
                    for t in range(CH)
                ],
            )
            return carry

        acc_near[...] = jnp.zeros_like(acc_near)
        lax.fori_loop(0, 2 * REACH + 1, step, 0)
        return acc_near[0:3, :] + acc_near[8:11, :]

    lax.fori_loop(0, KEEP // 4, target_build(0), 0)
    second = apply_near(f1, 1) - SHIFT * first
    fmat[6:9, :] = second
    keep_own(f2, second)
    send_all(f2, 2, False)
    send_all(f2, 2, True)
    lax.fori_loop(KEEP // 4, KEEP // 2, target_build(0), 0)
    lax.fori_loop(NEAR_SLOTS // 2, FAR_SLOTS // 2, last_terms, 0)
    third = apply_near(f2, 2) - SHIFT * second
    fmat[9:12, :] = third

    everything = fmat[...]
    local = lax.dot_general(
        fmat[0:24, :],
        everything,
        (((1,), (1,)), ((), ())),
        precision=HIGH,
        preferred_element_type=f32,
    )
    ga[zi] = local[0:8] + pltpu.roll(local[8:16], 32, 1) + pltpu.roll(local[16:24], 64, 1)

    def a_copy(d):
        q, h = ring_a[d - 1]
        return pltpu.make_async_remote_copy(
            src_ref=ga.at[zi],
            dst_ref=ga.at[zi],
            send_sem=a_send.at[d],
            recv_sem=a_recv.at[zi],
            device_id=(q, h),
            device_id_type=MESH,
        )

    def a_wait(d):
        slot = (zi + d) % RING
        pltpu.make_async_remote_copy(
            src_ref=ga.at[zi],
            dst_ref=ga.at[slot],
            send_sem=a_send.at[d],
            recv_sem=a_recv.at[slot],
            device_id=ring_a[d - 1],
            device_id_type=MESH,
        ).wait_recv()

    me_b = xi * NG + g

    def b_copy(i):
        return pltpu.make_async_remote_copy(
            src_ref=gb.at[me_b],
            dst_ref=gb.at[me_b],
            send_sem=b_send.at[i],
            recv_sem=b_recv.at[me_b],
            device_id=ring_b[i],
            device_id_type=MESH,
        )

    def b_wait(i):
        dx, dg = (i + 1) // NG, (i + 1) % NG
        slot = ((xi + dx) % 4) * NG + (g + dg) % NG
        pltpu.make_async_remote_copy(
            src_ref=gb.at[me_b],
            dst_ref=gb.at[slot],
            send_sem=b_send.at[i],
            recv_sem=b_recv.at[slot],
            device_id=ring_b[i],
            device_id_type=MESH,
        ).wait_recv()

    for d in range(1, RING):
        a_copy(d).start()

    acc_far[...] = jnp.zeros_like(acc_far)
    kept = KEEP // NG
    middle = KEEP + 2 * (FAR_SLOTS - KEEP) // 3
    lax.fori_loop(0, kept, target_apply(0), 0)
    lax.fori_loop(KEEP // 2, middle // 2, target_build(KEEP), 0)

    for d in range(1, RING):
        a_wait(d)
    part = ga[0]
    for i in range(1, RING):
        part = part + ga[i]
    gb[me_b] = part
    for i in range(RING - 1):
        b_copy(i).start()

    lax.fori_loop(middle // 2, FAR_SLOTS // 2, target_build(KEEP), 0)
    for o in (FAR, -FAR):
        for h in range(NG):

            @pl.when(valid(o))
            def _():
                wait_block(f1, 1, o, h)
                wait_block(f2, 2, o, h)

    lax.fori_loop(kept, 2 * FAR + 1, target_apply(kept), 0)
    mmat[0:16, :] = acc_far[0:16, :] + acc_far[16:32, :]

    for i in range(RING - 1):
        b_wait(i)
    whole = gb[0]
    for i in range(1, RING):
        whole = whole + gb[i]
    few = lax.broadcasted_iota(jnp.int32, (8, LANE), 1) < 24
    parts = [whole, pltpu.roll(whole, LANE - 32, 1), pltpu.roll(whole, LANE - 64, 1)]
    parts = [jnp.where(few, part, 0.0) for part in parts]
    gram = jnp.concatenate(parts, axis=0)
    head, tail = coefficients(gram)
    weights = jnp.dot(
        head[:, 0:24], fmat[0:24, :], precision=HIGH, preferred_element_type=f32
    )
    out_ref[:, 0:OWN] = weights
    out_ref[:, OWN + TGT :] = pltpu.roll(tail, LANE - 12, 1)
    both = head + pltpu.roll(tail, 12, 1)
    mapped = jnp.dot(
        both[:, 0:32], mmat[0:32, :], precision=HIGH, preferred_element_type=f32
    )
    out_ref[:, OWN : OWN + TGT] = mapped

    wait_send_all(c0, 0)
    wait_send_all(f1, 1)
    wait_send_all(f2, 2)
    for d in range(1, RING):
        a_copy(d).wait_send()
    for i in range(RING - 1):
        b_copy(i).wait_send()


def unpack(packed_ref, weights_ref, poly_ref, mapped_ref):
    weights_ref[...] = packed_ref[0:3, 0:OWN]
    mapped_ref[...] = packed_ref[0:3, OWN : OWN + TGT]
    poly_ref[...] = packed_ref[0:3, OWN + TGT : OWN + TGT + 4]


def shards(source_coords, source_values, target_coords, target_owner):
    vmem = pl.BlockSpec(memory_space=pltpu.VMEM)
    dma = pltpu.SemaphoreType.DMA
    packed = pl.pallas_call(
        kernel,
        out_shape=jax.ShapeDtypeStruct((8, OWN + TGT + LANE), f32),
        in_specs=[vmem] * 4,
        out_specs=vmem,
        scratch_shapes=[
            pltpu.VMEM((FAR_SLOTS, 32, LANE), f32),
            pltpu.VMEM((FAR_SLOTS, 16, LANE), f32),
            pltpu.VMEM((FAR_SLOTS, 16, LANE), f32),
            pltpu.VMEM((NEAR_SLOTS * OWN, OWN), bf16),
            pltpu.VMEM((NEAR_SLOTS * OWN, OWN), bf16),
            pltpu.VMEM((KEEP * OWN, TGT), bf16),
            pltpu.VMEM((KEEP * OWN, TGT), bf16),
            pltpu.VMEM((16, OWN), f32),
            pltpu.VMEM((32, TGT), f32),
            pltpu.VMEM((FAR_SLOTS // 2 * OWN, TERMS), bf16),
            pltpu.VMEM((FAR_SLOTS // 2 * OWN, TERMS), bf16),
            pltpu.VMEM((CH * TERMS, LANE), f32),
            pltpu.VMEM((CH * TERMS, LANE), f32),
            pltpu.VMEM((TERMS, OWN), bf16),
            pltpu.VMEM((2 * FAR + 1, TERMS, TGT), bf16),
            pltpu.VMEM((LANE, OWN), f32),
            pltpu.VMEM((LANE, TGT), f32),
            pltpu.VMEM((RING, 8, LANE), f32),
            pltpu.VMEM((RING, 8, LANE), f32),
            dma((3, FAR_SLOTS)),
            dma((3, FAR_SLOTS)),
            dma((RING,)),
            dma((RING,)),
            dma((RING,)),
            dma((RING,)),
        ],
        compiler_params=pltpu.CompilerParams(
            collective_id=0,
            has_side_effects=True,
            vmem_limit_bytes=62 * 1024 * 1024
        ),
    )(source_coords, source_values, target_coords, target_owner.reshape(1, TGT))
    return pl.pallas_call(
        unpack,
        out_shape=(
            jax.ShapeDtypeStruct((3, OWN), f32),
            jax.ShapeDtypeStruct((3, 4), f32),
            jax.ShapeDtypeStruct((3, TGT), f32),
        ),
        in_specs=[vmem],
        out_specs=(vmem,) * 3,
    )(packed)


def solution(mesh):
    both = ("blk", "grp")
    return jax.shard_map(
        shards,
        mesh=mesh,
        in_specs=(P(None, both), P(None, both), P(None, both), P(both)),
        out_specs=(P(None, both), P(), P(None, both)),
        check_vma=False,
    )
```

```python
import functools
import math

import jax
import jax.numpy as jnp
from jax import lax
from jax.experimental import pallas as pl
from jax.experimental.pallas import tpu as pltpu
from jax.sharding import PartitionSpec as P

MESH = pl.DeviceIdType.MESH
ITERS = 3
REACH = 2
FAR = REACH + 1
NB = 64
NG = 4
RING = 16
OWN = 640
TGT = 512
LANE = 128
CH = OWN // LANE
SLAB = OWN * NG
NSRC = SLAB * NB
STRETCH = 4.0 * SLAB
SHIFT = 2.0
TINY = 1e-6
LOG2E = 1.4426950408889634
XSCALE = math.sqrt(0.6 * LOG2E)
GRID = math.sqrt(STRETCH * LOG2E / 4.0)
TERMS = 48
ROOT = 1.0 / math.sqrt(NSRC)
NEAR_SLOTS = (2 * REACH + 1) * NG
FAR_SLOTS = (2 * FAR + 1) * NG
KEEP = 16
f32 = jnp.float32
bf16 = jnp.bfloat16
HIGH = lax.Precision.HIGHEST


def split(v):
    hi = v.astype(bf16)
    return hi, (v - hi.astype(f32)).astype(bf16)


def least_squares(hessenberg, beta):
    count = len(hessenberg)
    right_side = [beta] + [jnp.zeros_like(beta) for k in range(count)]
    upper = []
    cosines = []
    sines = []
    for k in range(count):
        column = list(hessenberg[k])
        for i in range(k):
            top = cosines[i] * column[i] + sines[i] * column[i + 1]
            lower = -sines[i] * column[i] + cosines[i] * column[i + 1]
            column[i] = top
            column[i + 1] = lower
        radius = jnp.sqrt(column[k] * column[k] + column[k + 1] * column[k + 1])
        cosine = column[k] / radius
        sine = column[k + 1] / radius
        column[k] = radius
        cosines.append(cosine)
        sines.append(sine)
        right_side[k + 1] = -sine * right_side[k]
        right_side[k] = cosine * right_side[k]
        upper.append(column[: k + 1])
    solved = [None] * count
    for k in reversed(range(count)):
        running = right_side[k]
        for j in range(k + 1, count):
            running = running - upper[j][k] * solved[j]
        solved[k] = running / upper[k][k]
    return solved


def pieces(v, count):
    out = []
    for i in range(count):
        part = v.astype(bf16).astype(f32)
        out.append(part)
        v = v - part
    return out


def point_terms(x, y, z, column, extra):
    one = jnp.ones_like(x)
    big = 1.0 if column else 8.0
    fine = []
    coarse = []
    scalar = -x * x
    whole = jnp.zeros_like(x)
    for v in (y, z):
        u = (v - 0.5) * GRID
        n = jnp.floor(u + 0.5)
        f = u - n
        f1, f2, f3 = pieces(f, 3)
        if column:
            fine += [f1, f2, f3, n, n, n, f1, f1, f2, f2]
        else:
            n8 = 8.0 * n
            fine += [n8, n8, n8, 8.0 * f1, 8.0 * f2, 8.0 * f3, 8.0 * f1, 8.0 * f2, 8.0 * f1, 8.0 * f2]
        coarse.append(n * big)
        scalar = scalar - (8.0 * n + 4.0 * f) * f
        whole = whole - 4.0 * n * n
    s = pieces(scalar, 3)
    w = pieces(whole, 2)
    x1, x2, x3 = pieces(x, 3)
    if column:
        fine += s + [one, one, one] + [x1, x1, x2, x2, x1, x3]
        coarse += w + [one, one, one]
    else:
        fine += [one, one, one] + s + [2.0 * v for v in (x1, x2, x1, x2, x3, x1)]
        coarse += [one, one] + w + [extra]
    return fine + coarse


def basis_rows(x, y, z):
    return (
        jnp.full_like(x, ROOT),
        (2.0 * x / NB - 1.0) * ROOT,
        (2.0 * y - 1.0) * ROOT,
        (2.0 * z - 1.0) * ROOT,
    )


def coefficients(gram):
    lane = lax.broadcasted_iota(jnp.int32, (8, LANE), 1)
    row = lax.broadcasted_iota(jnp.int32, (8, LANE), 0)
    tail_lanes = (lane >= 12) & (lane < 16)

    def total(v):
        return jnp.sum(v, axis=1, keepdims=True)

    def times_gram(v):
        return jnp.dot(v[:, 0:24], gram, precision=HIGH, preferred_element_type=f32)

    def shifted(v):
        up = pltpu.roll(v, 3, 1)
        across = pltpu.roll(v, 4, 1)
        moved = jnp.where(lane < 12, up, jnp.where((lane >= 16) & (lane < 20), across, 0.0))
        moved = jnp.where(lane < 3, 0.0, moved)
        return moved + SHIFT * v

    first = jnp.where((lane == row) & (row < 3), 1.0, 0.0)
    first_gram = times_gram(first)
    beta = jnp.sqrt(total(first_gram * first) + TINY)
    heads = [first / beta]
    tails = [jnp.zeros_like(first)]
    grams = [first_gram / beta]
    hessenberg = []
    for k in range(ITERS):
        head = shifted(heads[k]) + tails[k]
        tail = jnp.where(tail_lanes, grams[k], 0.0)
        head_gram = times_gram(head)
        column = [
            total(head_gram * heads[i]) + total(tail * tails[i]) for i in range(k + 1)
        ]
        for i in range(k + 1):
            head = head - column[i] * heads[i]
            tail = tail - column[i] * tails[i]
        rest_gram = head_gram
        for i in range(k + 1):
            rest_gram = rest_gram - column[i] * grams[i]
        length = jnp.sqrt(total(rest_gram * head) + total(tail * tail) + TINY)
        column.append(length)
        hessenberg.append(column)
        heads.append(head / length)
        tails.append(tail / length)
        grams.append(rest_gram / length)
    solved = least_squares(hessenberg, beta)
    head = solved[0] * heads[0]
    tail = solved[0] * tails[0]
    for k in range(1, ITERS):
        head = head + solved[k] * heads[k]
        tail = tail + solved[k] * tails[k]
    return head, tail


def kernel(
    coords_ref,
    values_ref,
    tcoords_ref,
    owner_ref,
    out_ref,
    c0,
    f1,
    f2,
    kh,
    kl,
    th,
    tl,
    acc_near,
    acc_far,
    lt_even,
    lt_odd,
    stage_even,
    stage_odd,
    rsrc,
    rtgt,
    fmat,
    mmat,
    ga,
    gb,
    send_sem,
    recv_sem,
    a_send,
    a_recv,
    b_send,
    b_recv,
):
    p = lax.axis_index("blk")
    g = lax.axis_index("grp")
    xi = p // RING
    zi = p % RING
    own = FAR * NG + g

    def valid(o):
        return (p + o >= 0) & (p + o < NB)

    halo = []
    for d in range(1, NG):
        halo.append((0, (g + d) % NG))
    for dist in range(1, FAR + 1):
        for o in (dist, -dist):
            for d in range(NG):
                halo.append((o, (g + d) % NG))
    ring_a = [(xi * RING + (zi + d) % RING, g) for d in range(1, RING)]
    ring_b = [
        (((xi + dx) % 4) * RING + zi, (g + dg) % NG)
        for dx in range(4)
        for dg in range(NG)
        if (dx, dg) != (0, 0)
    ]

    barrier = pltpu.get_barrier_semaphore()

    def signal(q, h):
        pl.semaphore_signal(barrier, inc=1, device_id=(q, h), device_id_type=MESH)

    expected = NG - 1 + len(ring_a) + len(ring_b)
    for o, h in halo:
        if o == 0:
            signal(p, h)
        else:
            pl.when(valid(o))(functools.partial(signal, p + o, h))
    for o in range(-FAR, FAR + 1):
        if o != 0:
            expected = expected + jnp.where(valid(o), NG, 0)
    for q, h in ring_a + ring_b:
        signal(q, h)

    for t in range(CH):
        lanes = slice(t * LANE, (t + 1) * LANE)
        c0[own, 3 * t : 3 * t + 3, :] = coords_ref[:, lanes]
        c0[own, 16 + 3 * t : 16 + 3 * t + 3, :] = values_ref[:, lanes]
    absent = jnp.where(
        lax.broadcasted_iota(jnp.int32, (32, LANE), 0) % 3 == 0, 1e5, 0.0
    )
    absent = jnp.where(lax.broadcasted_iota(jnp.int32, (32, LANE), 0) < 15, absent, 0.0)
    for o in range(-FAR, FAR + 1):
        if o != 0:

            @pl.when(jnp.logical_not(valid(o)))
            def _():
                for h in range(NG):
                    slot = (FAR + o) * NG + h
                    c0[slot] = absent
                    f1[slot] = jnp.zeros((16, LANE), f32)
                    f2[slot] = jnp.zeros((16, LANE), f32)

    pl.semaphore_wait(barrier, expected)

    def block_copy(buf, which, o, h):
        return pltpu.make_async_remote_copy(
            src_ref=buf.at[own],
            dst_ref=buf.at[(FAR - o) * NG + g],
            send_sem=send_sem.at[which, (FAR + o) * NG + h],
            recv_sem=recv_sem.at[which, (FAR - o) * NG + g],
            device_id=(p + o, h),
            device_id_type=MESH,
        )

    def send_all(buf, which, far):
        for o, h in halo:
            if (abs(o) == FAR) != far:
                continue
            copy = block_copy(buf, which, o, h)
            if o == 0:
                copy.start()
            else:
                pl.when(valid(o))(copy.start)

    def wait_send_all(buf, which):
        for o, h in halo:
            copy = block_copy(buf, which, o, h)
            if o == 0:
                copy.wait_send()
            else:
                pl.when(valid(o))(copy.wait_send)

    def wait_block(buf, which, o, h):
        slot = (FAR + o) * NG + h
        pltpu.make_async_remote_copy(
            src_ref=buf.at[own],
            dst_ref=buf.at[slot],
            send_sem=send_sem.at[which, slot],
            recv_sem=recv_sem.at[which, slot],
            device_id=(p + o, h),
            device_id_type=MESH,
        ).wait_recv()

    def place(k):
        oi = lax.div(k, NG)
        dist = lax.div(oi + 1, 2)
        o = jnp.where(lax.rem(oi, 2) == 1, dist, -dist)
        h = lax.rem(g + k, NG)
        return o, h, (FAR + o) * NG + h

    send_all(c0, 0, False)

    base = p.astype(f32)
    sx, sy, sz = coords_ref[0:1, :], coords_ref[1:2, :], coords_ref[2:3, :]
    source_terms = point_terms((sx - base) * XSCALE, sy, sz, False, jnp.zeros_like(sx))
    source_terms += [jnp.zeros_like(sx)] * (TERMS - len(source_terms))
    rsrc[...] = jnp.concatenate(source_terms, axis=0).astype(bf16)
    for stage in (stage_even, stage_odd):
        stage[...] = jnp.zeros_like(stage)
    sides = ((lt_even, stage_even), (lt_odd, stage_odd))
    fmat[...] = jnp.zeros_like(fmat)
    mmat[...] = jnp.zeros_like(mmat)
    fmat[0:3, :] = values_ref[...]
    for i, part in enumerate(basis_rows(sx, sy, sz)):
        fmat[12 + i : 13 + i, :] = part
    tx, ty, tz = tcoords_ref[0:1, :], tcoords_ref[1:2, :], tcoords_ref[2:3, :]
    owner = owner_ref[...]
    target_terms = point_terms((tx - base) * XSCALE, ty, tz, False, jnp.zeros_like(tx))
    masked = len(target_terms) - 1
    target_terms += [jnp.zeros_like(tx)] * (TERMS - len(target_terms))
    target_terms = jnp.concatenate(target_terms, axis=0)
    at_mask = lax.broadcasted_iota(jnp.int32, (TERMS, TGT), 0) == masked
    for o in range(-FAR, FAR + 1):
        mask = jnp.where(jnp.abs(owner - (p + o)) <= REACH, 0.0, -1e6)
        rtgt[FAR + o] = jnp.where(at_mask, mask, target_terms).astype(bf16)
    for i, part in enumerate(basis_rows(tx, ty, tz)):
        mmat[24 + i : 25 + i, :] = part


    def column_terms(slot, pair, side):
        lt, stage = sides[side]
        x, y, z = (c0[slot, pl.ds(i, CH, stride=3), :] for i in range(3))
        for i, v in enumerate(point_terms((x - base) * XSCALE, y, z, True, None)):
            stage[pl.ds(i, CH, stride=TERMS), :] = v
        for t in range(CH):
            at = pl.ds(pl.multiple_of(pair * OWN, OWN) + t * LANE, LANE)
            lt[at, :] = stage[t * TERMS : (t + 1) * TERMS, :].T.astype(bf16)

    def fill(pair, side, right, hi_ref, lo_ref, start):
        for t in range(CH):
            at = pl.ds(pl.multiple_of(pair * OWN, OWN) + t * LANE, LANE)
            put = pl.ds(start + t * LANE, LANE)
            e = jnp.exp2(jnp.dot(sides[side][0][at, :], right, preferred_element_type=f32))
            hi_ref[put, :], lo_ref[put, :] = split(e)

    def near_values(slot, t):
        cc = c0[slot, 3 * t : 3 * t + 3, :]
        parts = [c0[slot, 16 + 3 * t : 16 + 3 * t + 3, :]]
        parts += basis_rows(cc[0:1], cc[1:2], cc[2:3])
        parts.append(jnp.zeros((1, LANE), f32))
        return jnp.concatenate(split(jnp.concatenate(parts, axis=0)), axis=0)

    def arrived(k, last):
        o, h, slot = place(jnp.minimum(k, last))

        @pl.when((k <= last) & valid(o))
        def _():
            wait_block(c0, 0, o, h)

        return slot

    def build(pair, carry):
        odd = arrived(2 * pair + 1, NEAR_SLOTS - 1)
        even = arrived(2 * pair + 2, NEAR_SLOTS - 1)
        start = pl.multiple_of(pair * 2 * OWN, 2 * OWN)
        column_terms(odd, pair, 1)
        fill(pair, 0, rsrc[...], kh, kl, start)
        column_terms(even, pair + 1, 0)
        fill(pair, 1, rsrc[...], kh, kl, start + OWN)
        return carry

    column_terms(own, 0, 0)
    lax.fori_loop(0, NEAR_SLOTS // 2, build, 0)

    def blocks(m):
        return place(m * NG)[0], [place(m * NG + i)[2] for i in range(NG)]

    def product(hi_ref, lo_ref, region, values):
        v = jnp.concatenate(values, axis=1)
        at = pl.ds(pl.multiple_of(region * SLAB, SLAB), SLAB)
        return jnp.dot(v, hi_ref[at, :], preferred_element_type=f32) + jnp.dot(
            v, lo_ref[at, :], preferred_element_type=f32
        )

    def apply_first(m, carry):
        slots = blocks(m)[1]
        acc_near[...] += product(
            kh, kl, m, [near_values(slot, t) for slot in slots for t in range(CH)]
        )
        return carry

    acc_near[...] = jnp.zeros_like(acc_near)
    lax.fori_loop(0, 2 * REACH + 1, apply_first, 0)
    acc = acc_near[...]
    image = acc[0:8] + acc[8:16]
    first = image[0:3] - SHIFT * fmat[0:3, :]
    fmat[3:6, :] = first
    fmat[16:20, :] = image[3:7] - SHIFT * fmat[12:16, :]

    def keep_own(buf, v):
        for t in range(CH):
            buf[own, 3 * t : 3 * t + 3, :] = v[:, t * LANE : (t + 1) * LANE]

    keep_own(f1, first)
    send_all(f1, 1, False)
    send_all(c0, 0, True)
    send_all(f1, 1, True)

    def far_values(slot, t):
        cc = c0[slot, 3 * t : 3 * t + 3, :]
        parts = [
            c0[slot, 16 + 3 * t : 16 + 3 * t + 3, :],
            f1[slot, 3 * t : 3 * t + 3, :],
            f2[slot, 3 * t : 3 * t + 3, :],
            jnp.zeros((3, LANE), f32),
        ]
        parts += basis_rows(cc[0:1], cc[1:2], cc[2:3])
        return jnp.concatenate(split(jnp.concatenate(parts, axis=0)), axis=0)

    def target_build(first):
        def step(pair, carry):
            start = pl.multiple_of((2 * pair - first) * OWN, 2 * OWN)
            right = rtgt[FAR + place(2 * pair)[0]]
            fill(pair, 0, right, th, tl, start)
            fill(pair, 1, right, th, tl, start + OWN)
            return carry

        return step

    def target_apply(first):
        def step(m, carry):
            slots = blocks(m)[1]
            acc_far[...] += product(
                th,
                tl,
                m - first,
                [far_values(slot, t) for slot in slots for t in range(CH)],
            )
            return carry

        return step

    def last_terms(pair, carry):
        even = arrived(2 * pair, FAR_SLOTS - 1)
        odd = arrived(2 * pair + 1, FAR_SLOTS - 1)
        column_terms(even, pair, 0)
        column_terms(odd, pair, 1)
        return carry

    def padded_split(v):
        v = jnp.concatenate([v, jnp.zeros((5, LANE), f32)], axis=0)
        return jnp.concatenate(split(v), axis=0)

    def apply_near(buf, which):
        def step(m, carry):
            o, slots = blocks(m)
            for i in range(NG):
                h = place(m * NG + i)[1]

                @pl.when((m * NG + i > 0) & valid(o))
                def _():
                    wait_block(buf, which, o, h)

            acc_near[...] += product(
                kh,
                kl,
                m,
                [
                    padded_split(buf[slot, 3 * t : 3 * t + 3, :])
                    for slot in slots
                    for t in range(CH)
                ],
            )
            return carry

        acc_near[...] = jnp.zeros_like(acc_near)
        lax.fori_loop(0, 2 * REACH + 1, step, 0)
        return acc_near[0:3, :] + acc_near[8:11, :]

    lax.fori_loop(0, KEEP // 4, target_build(0), 0)
    second = apply_near(f1, 1) - SHIFT * first
    fmat[6:9, :] = second
    keep_own(f2, second)
    send_all(f2, 2, False)
    send_all(f2, 2, True)
    lax.fori_loop(KEEP // 4, KEEP // 2, target_build(0), 0)
    lax.fori_loop(NEAR_SLOTS // 2, FAR_SLOTS // 2, last_terms, 0)
    third = apply_near(f2, 2) - SHIFT * second
    fmat[9:12, :] = third

    everything = fmat[...]
    local = lax.dot_general(
        fmat[0:24, :],
        everything,
        (((1,), (1,)), ((), ())),
        precision=HIGH,
        preferred_element_type=f32,
    )
    ga[zi] = local[0:8] + pltpu.roll(local[8:16], 32, 1) + pltpu.roll(local[16:24], 64, 1)

    def a_copy(d):
        q, h = ring_a[d - 1]
        return pltpu.make_async_remote_copy(
            src_ref=ga.at[zi],
            dst_ref=ga.at[zi],
            send_sem=a_send.at[d],
            recv_sem=a_recv.at[zi],
            device_id=(q, h),
            device_id_type=MESH,
        )

    def a_wait(d):
        slot = (zi + d) % RING
        pltpu.make_async_remote_copy(
            src_ref=ga.at[zi],
            dst_ref=ga.at[slot],
            send_sem=a_send.at[d],
            recv_sem=a_recv.at[slot],
            device_id=ring_a[d - 1],
            device_id_type=MESH,
        ).wait_recv()

    me_b = xi * NG + g

    def b_copy(i):
        return pltpu.make_async_remote_copy(
            src_ref=gb.at[me_b],
            dst_ref=gb.at[me_b],
            send_sem=b_send.at[i],
            recv_sem=b_recv.at[me_b],
            device_id=ring_b[i],
            device_id_type=MESH,
        )

    def b_wait(i):
        dx, dg = (i + 1) // NG, (i + 1) % NG
        slot = ((xi + dx) % 4) * NG + (g + dg) % NG
        pltpu.make_async_remote_copy(
            src_ref=gb.at[me_b],
            dst_ref=gb.at[slot],
            send_sem=b_send.at[i],
            recv_sem=b_recv.at[slot],
            device_id=ring_b[i],
            device_id_type=MESH,
        ).wait_recv()

    for d in sorted(range(1, RING), key=lambda d: -min(d, RING - d)):
        a_copy(d).start()

    acc_far[...] = jnp.zeros_like(acc_far)
    kept = KEEP // NG
    middle = KEEP + (FAR_SLOTS - KEEP) // 2
    lax.fori_loop(0, kept, target_apply(0), 0)
    lax.fori_loop(KEEP // 2, middle // 2, target_build(KEEP), 0)

    for d in range(1, RING):
        a_wait(d)
    part = ga[0]
    for i in range(1, RING):
        part = part + ga[i]
    gb[me_b] = part
    def b_hops(i):
        dx, dg = (i + 1) // NG, (i + 1) % NG
        return min(dx, 4 - dx) + min(dg, NG - dg)

    for i in sorted(range(RING - 1), key=lambda i: -b_hops(i)):
        b_copy(i).start()

    lax.fori_loop(middle // 2, FAR_SLOTS // 2, target_build(KEEP), 0)
    for o in (FAR, -FAR):
        for h in range(NG):

            @pl.when(valid(o))
            def _():
                wait_block(f1, 1, o, h)
                wait_block(f2, 2, o, h)

    lax.fori_loop(kept, 2 * FAR + 1, target_apply(kept), 0)
    mmat[0:16, :] = acc_far[0:16, :] + acc_far[16:32, :]

    for i in range(RING - 1):
        b_wait(i)
    whole = gb[0]
    for i in range(1, RING):
        whole = whole + gb[i]
    few = lax.broadcasted_iota(jnp.int32, (8, LANE), 1) < 24
    parts = [whole, pltpu.roll(whole, LANE - 32, 1), pltpu.roll(whole, LANE - 64, 1)]
    parts = [jnp.where(few, part, 0.0) for part in parts]
    gram = jnp.concatenate(parts, axis=0)
    head, tail = coefficients(gram)
    weights = jnp.dot(
        head[:, 0:24], fmat[0:24, :], precision=HIGH, preferred_element_type=f32
    )
    out_ref[:, 0:OWN] = weights
    out_ref[:, OWN + TGT :] = pltpu.roll(tail, LANE - 12, 1)
    both = head + pltpu.roll(tail, 12, 1)
    mapped = jnp.dot(
        both[:, 0:32], mmat[0:32, :], precision=HIGH, preferred_element_type=f32
    )
    out_ref[:, OWN : OWN + TGT] = mapped

    wait_send_all(c0, 0)
    wait_send_all(f1, 1)
    wait_send_all(f2, 2)
    for d in range(1, RING):
        a_copy(d).wait_send()
    for i in range(RING - 1):
        b_copy(i).wait_send()


def unpack(packed_ref, weights_ref, poly_ref, mapped_ref):
    weights_ref[...] = packed_ref[0:3, 0:OWN]
    mapped_ref[...] = packed_ref[0:3, OWN : OWN + TGT]
    poly_ref[...] = packed_ref[0:3, OWN + TGT : OWN + TGT + 4]


def shards(source_coords, source_values, target_coords, target_owner):
    vmem = pl.BlockSpec(memory_space=pltpu.VMEM)
    dma = pltpu.SemaphoreType.DMA
    packed = pl.pallas_call(
        kernel,
        out_shape=jax.ShapeDtypeStruct((8, OWN + TGT + LANE), f32),
        in_specs=[vmem] * 4,
        out_specs=vmem,
        scratch_shapes=[
            pltpu.VMEM((FAR_SLOTS, 32, LANE), f32),
            pltpu.VMEM((FAR_SLOTS, 16, LANE), f32),
            pltpu.VMEM((FAR_SLOTS, 16, LANE), f32),
            pltpu.VMEM((NEAR_SLOTS * OWN, OWN), bf16),
            pltpu.VMEM((NEAR_SLOTS * OWN, OWN), bf16),
            pltpu.VMEM((KEEP * OWN, TGT), bf16),
            pltpu.VMEM((KEEP * OWN, TGT), bf16),
            pltpu.VMEM((16, OWN), f32),
            pltpu.VMEM((32, TGT), f32),
            pltpu.VMEM((FAR_SLOTS // 2 * OWN, TERMS), bf16),
            pltpu.VMEM((FAR_SLOTS // 2 * OWN, TERMS), bf16),
            pltpu.VMEM((CH * TERMS, LANE), f32),
            pltpu.VMEM((CH * TERMS, LANE), f32),
            pltpu.VMEM((TERMS, OWN), bf16),
            pltpu.VMEM((2 * FAR + 1, TERMS, TGT), bf16),
            pltpu.VMEM((LANE, OWN), f32),
            pltpu.VMEM((LANE, TGT), f32),
            pltpu.VMEM((RING, 8, LANE), f32),
            pltpu.VMEM((RING, 8, LANE), f32),
            dma((3, FAR_SLOTS)),
            dma((3, FAR_SLOTS)),
            dma((RING,)),
            dma((RING,)),
            dma((RING,)),
            dma((RING,)),
        ],
        compiler_params=pltpu.CompilerParams(
            collective_id=0,
            has_side_effects=True,
            vmem_limit_bytes=62 * 1024 * 1024
        ),
    )(source_coords, source_values, target_coords, target_owner.reshape(1, TGT))
    return pl.pallas_call(
        unpack,
        out_shape=(
            jax.ShapeDtypeStruct((3, OWN), f32),
            jax.ShapeDtypeStruct((3, 4), f32),
            jax.ShapeDtypeStruct((3, TGT), f32),
        ),
        in_specs=[vmem],
        out_specs=(vmem,) * 3,
    )(packed)


def solution(mesh):
    both = ("blk", "grp")
    return jax.shard_map(
        shards,
        mesh=mesh,
        in_specs=(P(None, both), P(None, both), P(None, both), P(both)),
        out_specs=(P(None, both), P(), P(None, both)),
        check_vma=False,
    )
```
